256 devices in a mesh: row: 32 (over x, y, core), col: 8 (over z).
Axes of the slice: x: 4, y: 4, z: 8, core: 2. Of those that a mesh axis runs over, the one named last changes fastest.
Arguments:
- state: float32 [9, 35, 65536], P(None, None, ('col', 'row')), may hold values from -6 to 6
- geometry: bfloat16 [9, 128, 65536], P(None, 'row', 'col'), may hold values from -5 to 5
- material: float32 [4, 65536], P(None, ('col', 'row')), may hold values from 0.5 to 2
- neighbours: int32 [4, 4, 65536], P(None, None, ('col', 'row')), may hold values from 0 to 1023, as said below
- send_faces: int32 [256, 8, 64], P(('col', 'row')), may hold values from 0 to 1023, as said below
- vol_eval: float32 [35, 128], replicated, may hold values from -1 to 1
- vol_grad: bfloat16 [3, 35, 128], replicated, may hold values from -0.3125 to 0.3125
- face_eval: float32 [4, 35, 27], replicated, may hold values from -1 to 1
- face_lift: float32 [4, 35, 27], replicated, may hold values from -0.625 to 0.625
- normals: bfloat16 [3, 27, 4, 65536], P(None, None, None, ('col', 'row')), may hold values from -5 to 5
- areas: float32 [27, 4, 65536], P(None, None, ('col', 'row')), may hold values from 0.5 to 2
Outputs:
- section: float32 [9, 35, 65536], P(None, None, ('col', 'row'))
The draws below stay inside these ranges and needn't reach their ends.
Inputs may be any that keep to these rules, and one draw needn't show every extreme that they name: `neighbours`: field 0 is the kind: 0 the neighbour face lies in the same block, 1 in another block of the same row group, 2 free surface, 3 absorbing. Field 1 is the neighbour block's col index (the own col index for kinds 0, 2, 3). Field 2 is, for kind 0, the neighbour's face number f * 256 + e within the block; for kind 1, a slot below the number of faces that the neighbour's block lists for this block in send_faces; else 0. Field 3 is an orientation of 0 to 2 (0 for kinds 2 and 3). Neighbouring is mutual: the neighbour face names this face back, with orientation (3 - turn) % 3. `send_faces`: A block lists at most 64 faces for one col index, the same number as that block lists back, and nothing for its own col index; entries past the count are 0. In every row group some pair of blocks lists exactly 64 faces to each other.
All inputs are finite; a program needn't handle non-finite values.
Results may differ from the reference program's by a relative error of at most 0.0065.
Values may be sent and summed in bfloat16 or wider, within the bound.
A program may use at most 64 MiB of HBM per device.

```python
import math
import jax
import jax.numpy as jnp
from jax import lax

NQ = 9
NB = 35
VQ = 128
FQ = 27
E_DEV = 256
SLOTS = 64
ELEMENTS = 65536
N_ROW = 32
N_COL = 8


def build_faces(key):
    face_count = 4 * E_DEV
    column_ids = jnp.arange(N_COL, dtype=jnp.int32)
    upper_half = column_ids[:, None] < column_ids[None, :]
    counts = jax.random.randint(jax.random.fold_in(key, 11), (N_ROW, N_COL, N_COL), SLOTS // 4, SLOTS + 1)
    counts = jnp.where(upper_half[None], counts, jnp.transpose(counts, (0, 2, 1)))
    first_col = jax.random.randint(jax.random.fold_in(key, 12), (N_ROW, 1, 1), 0, N_COL)
    second_col = (first_col + jax.random.randint(jax.random.fold_in(key, 13), (N_ROW, 1, 1), 1, N_COL)) % N_COL
    sender = column_ids[None, :, None]
    getter = column_ids[None, None, :]
    filled = (sender == first_col) & (getter == second_col) | (sender == second_col) & (getter == first_col)
    counts = jnp.where(filled, SLOTS, counts)
    counts = jnp.where(sender == getter, 0, counts).astype(jnp.int32)
    pair_turns = jax.random.randint(jax.random.fold_in(key, 14), (N_ROW, N_COL, N_COL, SLOTS), 0, 3)
    pair_turns = jnp.where(upper_half[None, :, :, None], pair_turns, (3 - jnp.transpose(pair_turns, (0, 2, 1, 3))) % 3)

    def one_device(row_id, column_id):
        device_key = jax.random.fold_in(jax.random.fold_in(key, 15), column_id * N_ROW + row_id)
        shuffle = jax.random.permutation(jax.random.fold_in(device_key, 1), face_count).astype(jnp.int32)
        own_counts = counts[row_id, column_id]
        list_ends = jnp.cumsum(own_counts)
        starts = list_ends - own_counts
        remote_total = list_ends[N_COL - 1]
        positions = jnp.arange(face_count, dtype=jnp.int32)
        peer_index = jnp.minimum(jnp.sum((list_ends[None, :] <= positions[:, None]).astype(jnp.int32), axis=1), N_COL - 1)
        slot_index = jnp.clip(positions - starts[peer_index], 0, SLOTS - 1)
        remote = positions < remote_total
        offset = positions - remote_total
        remaining = face_count - remote_total
        edge_total = jax.random.randint(jax.random.fold_in(device_key, 2), (), face_count // 16, face_count // 8 + 1)
        paired = 2 * ((remaining - edge_total) // 2)
        is_pair = (offset >= 0) & (offset < paired)
        partner = jnp.clip(remote_total + jnp.bitwise_xor(jnp.maximum(offset, 0), 1), 0, face_count - 1)
        local_turns = jax.random.randint(jax.random.fold_in(device_key, 3), (face_count,), 0, 3)
        base_turn = local_turns[jnp.clip(remote_total + offset - offset % 2, 0, face_count - 1)]
        pair_turn = jnp.where(offset % 2 == 0, base_turn, (3 - base_turn) % 3)
        edge_kind = 2 + jax.random.randint(jax.random.fold_in(device_key, 4), (face_count,), 0, 2)
        face_kind = jnp.where(remote, 1, jnp.where(is_pair, 0, edge_kind))
        peer_field = jnp.where(remote, peer_index, column_id)
        target = jnp.where(remote, slot_index, jnp.where(is_pair, shuffle[partner], 0))
        turning = jnp.where(remote, pair_turns[row_id, column_id, peer_index, slot_index], jnp.where(is_pair, pair_turn, 0))
        fields = jnp.stack([face_kind, peer_field, target, turning]).astype(jnp.int32)
        by_face = jnp.zeros((4, face_count), jnp.int32).at[:, shuffle].set(fields)
        slot_ids = jnp.arange(SLOTS, dtype=jnp.int32)
        spot_ids = jnp.clip(starts[:, None] + slot_ids[None, :], 0, face_count - 1)
        send_rows = jnp.where(slot_ids[None, :] < own_counts[:, None], shuffle[spot_ids], 0)
        return (by_face.reshape(4, 4, E_DEV), send_rows.astype(jnp.int32))

    def one_column(column_id):

        def per_row(row_id):
            return one_device(row_id, column_id)
        return jax.vmap(per_row)(jnp.arange(N_ROW, dtype=jnp.int32))
    fields, send_rows = jax.vmap(one_column)(column_ids)
    links = jnp.transpose(fields, (2, 3, 0, 1, 4)).reshape(4, 4, N_COL * N_ROW * E_DEV)
    return (links, send_rows.reshape(N_COL * N_ROW, N_COL, SLOTS))


def draw_neighbours(key, part):
    return build_faces(key)[0]


def draw_send_faces(key, part):
    return build_faces(key)[1]


def shard_levels(own_key, shape, pieces, low, high):
    factor_of, own = 1.0, jax.random.fold_in(own_key, 6)
    for position, shards_of in pieces:
        draws = jnp.exp(jax.random.uniform(jax.random.fold_in(own, position), (shards_of,), jnp.float32, low / len(pieces), high / len(pieces)))
        factor_of = factor_of * jnp.repeat(draws, shape[position] // shards_of).reshape([-1 if axis == position else 1 for axis in range(len(shape))])
    return factor_of


def scatter_about(rng, shape, width, limit, split=(), held_as=jnp.bfloat16):
    loudness = shard_levels(rng, shape, split, -0.22, 0.18) if split else 1.0
    values = jax.random.normal(rng, shape, jnp.float32) * width * loudness
    return jnp.minimum(jnp.maximum(values, -limit), limit).astype(held_as)


def setup_inputs(seed: int = 0) -> dict:
    splits = jax.random.split(jax.random.key(seed), 12)
    state = scatter_about(splits[0], (NQ, NB, ELEMENTS), 1.0, 6.0, ((2, 256),), jnp.float32)
    geometry = scatter_about(splits[1], (9, VQ, ELEMENTS), 1.0, 5.0, ((1, 32), (2, 8)))
    material = jnp.clip(jnp.exp(math.log(2.0) - 1.3862944 * jax.random.uniform(splits[2], (4, ELEMENTS), jnp.float32) ** shard_levels(splits[2], (4, ELEMENTS), ((1, 256),), -0.2, 0.2)), 0.5, 2.0)
    neighbours = draw_neighbours(jax.random.fold_in(splits[11], 71), 0)
    send_faces = draw_send_faces(jax.random.fold_in(splits[11], 71), 0)
    vol_eval = scatter_about(splits[5], (NB, VQ), NB ** -0.5, 1.0, (), jnp.float32)
    vol_grad = scatter_about(splits[6], (3, NB, VQ), (3 * VQ) ** -0.5, 0.3125)
    face_eval = scatter_about(splits[7], (4, NB, FQ), NB ** -0.5, 1.0, (), jnp.float32)
    face_lift = scatter_about(splits[8], (4, NB, FQ), (4 * FQ) ** -0.5, 0.625, (), jnp.float32)
    normals = scatter_about(splits[9], (3, FQ, 4, ELEMENTS), 1.0, 5.0, ((3, 256),))
    areas = jnp.clip(jnp.exp(math.log(2.0) - 1.3862944 * jax.random.uniform(splits[10], (FQ, 4, ELEMENTS), jnp.float32) ** shard_levels(splits[10], (FQ, 4, ELEMENTS), ((2, 256),), -0.2, 0.2)), 0.5, 2.0)
    return {"state": state, "geometry": geometry, "material": material, "neighbours": neighbours, "send_faces": send_faces, "vol_eval": vol_eval, "vol_grad": vol_grad, "face_eval": face_eval, "face_lift": face_lift, "normals": normals, "areas": areas}


HIGHEST = lax.Precision.HIGHEST

def normal_flux(values, lame_first, rigidity, buoyancy, normal):
    velocity = values[6:9]
    stress = values[0:6]
    normal_speed = velocity[0] * normal[0] + velocity[1] * normal[1] + velocity[2] * normal[2]
    pressure = lame_first * normal_speed
    components = [-(pressure + 2.0 * rigidity * normal[0] * velocity[0]), -(pressure + 2.0 * rigidity * normal[1] * velocity[1]), -(pressure + 2.0 * rigidity * normal[2] * velocity[2]), -rigidity * (normal[0] * velocity[1] + normal[1] * velocity[0]), -rigidity * (normal[1] * velocity[2] + normal[2] * velocity[1]), -rigidity * (normal[0] * velocity[2] + normal[2] * velocity[0]), -buoyancy * (stress[0] * normal[0] + stress[3] * normal[1] + stress[5] * normal[2]), -buoyancy * (stress[3] * normal[0] + stress[1] * normal[1] + stress[4] * normal[2]), -buoyancy * (stress[5] * normal[0] + stress[4] * normal[1] + stress[2] * normal[2])]
    return jnp.stack(components)

def volume_fluxes(points, metric, material):
    values = points.astype(jnp.float32)
    result = []
    for direction in range(3):
        normal = (metric[3 * direction], metric[3 * direction + 1], metric[3 * direction + 2])
        result.append(normal_flux(values, material[0], material[1], material[2], normal))
    return jnp.stack(result).astype(jnp.bfloat16)

def rotate_points(gathered, turning):
    full_shape = gathered.shape
    grouped = gathered.reshape(full_shape[0], full_shape[1] // 3, 3, full_shape[2], full_shape[3])
    rotated_one = jnp.roll(grouped, -1, axis=2).reshape(full_shape)
    rotated_two = jnp.roll(grouped, -2, axis=2).reshape(full_shape)
    return jnp.where(turning == 0, gathered, jnp.where(turning == 1, rotated_one, rotated_two))

def exterior(traces, gathered, face_kind, turning):
    rotated = rotate_points(gathered, turning)
    mirror = jnp.concatenate([-traces[0:6], traces[6:9]], axis=0)
    return jnp.where(face_kind == 2, mirror, jnp.where(face_kind == 3, 0.0, rotated))

def face_flux(interior, exterior_trace, interior_material, exterior_material, normals, areas):
    normal = (normals[0], normals[1], normals[2])
    interior_flux = normal_flux(interior, interior_material[0], interior_material[1], interior_material[2], normal)
    exterior_flux = normal_flux(exterior_trace, exterior_material[0], exterior_material[1], exterior_material[2], normal)
    interior_speed = jnp.sqrt((interior_material[0] + 2.0 * interior_material[1]) * interior_material[2])
    exterior_speed = jnp.sqrt((exterior_material[0] + 2.0 * exterior_material[1]) * exterior_material[2])
    penalty = 0.5 * jnp.maximum(interior_speed, exterior_speed) * areas
    return 0.5 * (interior_flux + exterior_flux) + penalty * (interior - exterior_trace)

def reference(state, geometry, material, neighbours, send_faces, vol_eval, vol_grad, face_eval, face_lift, normals, areas):
    elem_total = state.shape[2]
    traces = jnp.einsum('fbq,mbe->mqfe', face_eval, state, precision=HIGHEST)
    flat_traces = traces.reshape(9, FQ, 4 * elem_total)
    block_count = N_ROW * N_COL

    def one_block(block_id):
        start = block_id * E_DEV
        column_id = block_id // N_ROW
        row_id = block_id % N_ROW
        own_state = lax.dynamic_slice_in_dim(state, start, E_DEV, 2)
        own_geometry = lax.dynamic_slice_in_dim(geometry, start, E_DEV, 2).astype(jnp.float32)
        own_material = lax.dynamic_slice_in_dim(material, start, E_DEV, 1)
        own_links = lax.dynamic_slice_in_dim(neighbours, start, E_DEV, 2)
        own_traces = lax.dynamic_slice_in_dim(traces, start, E_DEV, 3)
        own_normals = lax.dynamic_slice_in_dim(normals, start, E_DEV, 3).astype(jnp.float32)
        own_areas = lax.dynamic_slice_in_dim(areas, start, E_DEV, 2)
        points = jnp.einsum('bq,mbe->mqe', vol_eval, own_state, precision=HIGHEST).astype(jnp.bfloat16)
        fluxes = volume_fluxes(points, own_geometry, own_material)
        volume = jnp.einsum('dbq,dmqe->mbe', vol_grad.astype(jnp.float32), fluxes.astype(jnp.float32), precision=HIGHEST)
        face_kind = own_links[0]
        peer_index = own_links[1]
        target = own_links[2]
        turning = own_links[3]
        partner_block = (peer_index * N_ROW + row_id).astype(jnp.int32)
        listed = send_faces[partner_block, column_id, jnp.minimum(target, SLOTS - 1)]
        remote_face = listed // E_DEV
        remote_elem = partner_block * E_DEV + listed % E_DEV
        local_face = target // E_DEV
        local_elem = start + target % E_DEV
        own_face = jnp.broadcast_to(jnp.arange(4, dtype=jnp.int32)[:, None], (4, E_DEV))
        own_elem = jnp.broadcast_to(start + jnp.arange(E_DEV, dtype=jnp.int32)[None, :], (4, E_DEV))
        other_face = jnp.where(face_kind == 0, local_face, jnp.where(face_kind == 1, remote_face, own_face))
        other_elem = jnp.where(face_kind == 0, local_elem, jnp.where(face_kind == 1, remote_elem, own_elem))
        global_face = (other_face * elem_total + other_elem).astype(jnp.int32)
        gathered = jnp.take(flat_traces, global_face.reshape(-1), axis=2).reshape(own_traces.shape)
        other_material = jnp.take(material[0:3], other_elem.reshape(-1).astype(jnp.int32), axis=1).reshape(3, 1, 4, E_DEV)
        exterior_trace = exterior(own_traces, gathered, face_kind, turning)
        numeric_flux = face_flux(own_traces, exterior_trace, own_material[0:3][:, None, None, :], other_material, own_normals, own_areas)
        surface = jnp.einsum('fbq,mqfe->mbe', face_lift, numeric_flux, precision=HIGHEST)
        return own_state + own_material[3][None, None, :] * (volume - surface)
    sections = lax.map(one_block, jnp.arange(block_count, dtype=jnp.int32))
    return jnp.transpose(sections, (1, 2, 0, 3)).reshape(9, NB, elem_total)
```

```python
import jax
import jax.numpy as jnp
from jax import lax
from jax.experimental import pallas as pl
from jax.experimental.pallas import tpu as pltpu
from jax.sharding import PartitionSpec as P

MESH = pl.DeviceIdType.MESH
F32, BF16, I32 = jnp.float32, jnp.bfloat16, jnp.int32

NQ, NB, BP = 9, 35, 40
FQ, FACES, E = 27, 4, 256
ROWS, COLS, SLOTS = 32, 8, 64
LANES = 128
WIDE = NQ * LANES
KP = NQ * BP + 8
PITCH = 264


def iota(shape, dim):
    return lax.broadcasted_iota(I32, shape, dim)


def ones_where(mask):
    return jnp.where(mask, 1.0, 0.0).astype(BF16)


def mm(a, b):
    return jnp.dot(a, b, preferred_element_type=F32)


def mm_t(a, b):
    return lax.dot_general(a, b, (((1,), (1,)), ((), ())), preferred_element_type=F32)


def halves(x):
    return jnp.concatenate([x[:, :LANES], x[:, LANES:]], axis=0)


def steps(x, size, count):
    result = jnp.zeros_like(x)
    for k in range(1, count):
        result = result + jnp.where(x >= size * k, 1, 0)
    return result


def kernel(
    state, geometry, material, neighbours, send_faces, vol_eval, vol_grad, face_eval, face_lift,
    normals, areas, out,
    st_v, mat_v, nb_v, sf_v, ve_v, vg_v, fe_v, fl_v, nrm_v, ar_v,
    recv, sendb, xr, sp, sb, raw, ohs, tr, pts, own, gath, flx, fx, vgm,
    load_sem, gsend_sem, grecv_sem, tsend_sem, trecv_sem,
):
    row, col = lax.axis_index("row"), lax.axis_index("col")
    chip, core = row // 2, row % 2
    cx, cy = chip // 4, chip % 4

    pairs = [
        (state, st_v), (material, mat_v), (neighbours, nb_v), (send_faces, sf_v), (vol_eval, ve_v),
        (vol_grad, vg_v), (face_eval, fe_v), (face_lift, fl_v), (normals, nrm_v), (areas, ar_v),
    ]
    loads = [pltpu.make_async_copy(a, b, load_sem.at[i]) for i, (a, b) in enumerate(pairs)]
    for copy in loads:
        copy.start()

    def block(p):
        return geometry.at[:, pl.ds(2 * p, 2)]

    local = pltpu.make_async_copy(block(row), recv.at[row], grecv_sem.at[row])
    local.start()

    barrier = pltpu.get_barrier_semaphore()

    @pl.loop(1, ROWS)
    def _(d):
        pl.semaphore_signal(
            barrier, inc=1, device_id={"row": lax.rem(row + d, ROWS), "col": col}, device_id_type=MESH
        )

    @pl.loop(1, COLS)
    def _(d):
        pl.semaphore_signal(
            barrier, inc=1, device_id={"row": row, "col": lax.rem(col + d, COLS)}, device_id_type=MESH
        )

    def metric_copy(to, source):
        return pltpu.make_async_remote_copy(
            src_ref=block(to), dst_ref=recv.at[source], send_sem=gsend_sem.at[to],
            recv_sem=grecv_sem.at[source], device_id={"row": to, "col": col}, device_id_type=MESH,
        )

    def trace_copy(to, source):
        return pltpu.make_async_remote_copy(
            src_ref=sendb.at[to], dst_ref=xr.at[source], send_sem=tsend_sem.at[to],
            recv_sem=trecv_sem.at[source], device_id={"row": row, "col": to}, device_id_type=MESH,
        )

    def chip_at(o, sign):
        dx, dy = o // 4, o % 4
        return lax.rem(cx + sign * dx + 4, 4) * 4 + lax.rem(cy + sign * dy + 4, 4)

    for copy in loads:
        copy.wait()
    for m in range(NQ):
        sp[m * BP : m * BP + NB, :] = st_v[m]
        sp[m * BP + NB : (m + 1) * BP, :] = jnp.zeros((BP - NB, E), F32)
    high = mat_v[0:3, :].astype(BF16).astype(F32)
    sp[NQ * BP : NQ * BP + 3, :] = high
    sp[NQ * BP + 3 : NQ * BP + 6, :] = mat_v[0:3, :] - high
    sp[NQ * BP + 6 : KP, :] = jnp.zeros((2, E), F32)
    dof = sp[...].astype(BF16)

    raw[...] = jnp.zeros(raw.shape, F32)
    for q in range(FQ):
        for t in range(2):
            raw[0, 8 * q + 4 * t : 8 * q + 4 * t + 4, 0:NB] = fe_v[q]
            raw[1, 8 * q + 4 * t : 8 * q + 4 * t + 4, 0:NB] = fl_v[q]
    eval_rows = raw[0].astype(BF16)
    lift_rows = raw[1].astype(BF16)

    col_kp = iota((1, KP), 1)
    m_col = steps(col_kp, BP, NQ)
    spread9 = ones_where((iota((BP, 1), 0) == col_kp - BP * m_col) & (col_kp < NQ * BP))
    wide_eval = mm(eval_rows, spread9).astype(BF16)
    row_t = iota((256, 1), 0)
    m_row = steps(row_t, FQ, NQ)
    q_row = row_t - FQ * m_row
    same = (m_row == m_col) & (row_t < NQ * FQ) & (col_kp < NQ * BP)
    carry = (row_t - NQ * FQ == col_kp - NQ * BP) & (col_kp >= NQ * BP)
    for f in range(FACES):
        pick = ones_where(iota((1, 8 * FQ), 1) == 8 * q_row + f)
        weights = jnp.where(same, mm(pick, wide_eval), jnp.where(carry, 1.0, 0.0)).astype(BF16)
        tr[:, f * E : (f + 1) * E] = mm(weights, dof).astype(BF16)

    listed = jnp.transpose(jnp.concatenate([sf_v[0], sf_v[0]], axis=1))
    for p in range(COLS):
        ohs[p * SLOTS : (p + 1) * SLOTS, :] = ones_where(
            listed[0:SLOTS, p : p + 1] == iota((1, FACES * E), 1)
        )
    outgoing = mm_t(ohs[...], tr[...]).astype(BF16)
    for p in range(COLS):
        sendb[p] = outgoing[p * SLOTS : (p + 1) * SLOTS, :]
    xr[col] = jnp.zeros((SLOTS, 256), BF16)

    pl.semaphore_wait(barrier, ROWS + COLS - 2)

    metric_copy(2 * chip + (1 - core), row).start()

    @pl.loop(1, 16)
    def _(o):
        peer = chip_at(o, 1)
        metric_copy(2 * peer + core, row).start()
        metric_copy(2 * peer + (1 - core), row).start()

    @pl.loop(1, COLS)
    def _(d):
        trace_copy(lax.rem(col + d, COLS), col).start()

    for m in range(NQ):
        both = jnp.concatenate(
            [sp[m * BP : (m + 1) * BP, :LANES], sp[m * BP : (m + 1) * BP, LANES:]], axis=0
        )
        sb[:, m * LANES : (m + 1) * LANES] = both.astype(BF16)
    tile_col = jnp.where(iota((1, 2 * BP), 1) >= BP, 1, 0)
    twice = ones_where(iota((BP, 1), 0) == iota((1, 2 * BP), 1) - BP * tile_col)
    face_row = iota((8 * FQ, 1), 0)
    eval_mask = ((face_row >> 2) & 1) == tile_col
    face_weights = jnp.where(eval_mask, mm(eval_rows, twice), 0.0).astype(BF16)
    own[...] = mm(face_weights, sb[...]).reshape(FQ, 8, WIDE)
    point_row = iota((256, 1), 0)
    spread_v = ones_where(iota((1, 128), 1) == 4 * (point_row >> 3) + (point_row & 3))
    pad = jnp.zeros((BP - NB, 128), F32)
    eval2 = jnp.concatenate([ve_v[...], pad, ve_v[...], pad], axis=0).astype(BF16)
    vol_mask = ((point_row >> 2) & 1) == tile_col
    vol_weights = jnp.where(vol_mask, mm_t(spread_v, eval2), 0.0).astype(BF16)
    pts[...] = mm(vol_weights, sb[...])
    tile_row = jnp.where(iota((2 * BP, 1), 0) >= BP, 1, 0)
    grad_mask = tile_row == ((iota((1, 256), 1) >> 2) & 1)
    for d in range(3):
        grad = vg_v[d].astype(F32)
        grad2 = jnp.concatenate([grad, pad, grad, pad], axis=0).astype(BF16)
        vgm[:, d * 256 : (d + 1) * 256] = jnp.where(grad_mask, mm_t(grad2, spread_v), 0.0).astype(BF16)
    twice_t = ones_where(iota((2 * BP, 1), 0) - BP * tile_row == iota((1, BP), 1))
    lift_mask = tile_row == ((iota((1, 8 * FQ), 1) >> 2) & 1)
    lift = jnp.where(lift_mask, mm_t(twice_t, lift_rows), 0.0).astype(BF16)

    kind, peer, target, turn = nb_v[0], nb_v[1], nb_v[2], nb_v[3]
    face_id = iota((FACES, E), 0) * E + iota((FACES, E), 1)
    code = jnp.where(
        kind == 0, target, jnp.where(kind == 1, FACES * E + peer * SLOTS + target, face_id)
    )
    for f in range(FACES):
        got = mm(tr[...], ones_where(iota((FACES * E, 1), 0) == code[f : f + 1, :]))
        for t in range(2):
            gath[(4 * t + f) * PITCH : (4 * t + f) * PITCH + 256, :] = got[:, t * LANES : (t + 1) * LANES]

    @pl.loop(1, COLS)
    def _(d):
        source = lax.rem(col + COLS - d, COLS)
        trace_copy(source, source).wait_recv()

    ident = ones_where(iota((256, 1), 0) == iota((1, 256), 1))
    xt = mm_t(ident, xr[...].reshape(COLS * SLOTS, 256)).astype(BF16)
    for f in range(FACES):
        got = mm(xt, ones_where(iota((COLS * SLOTS, 1), 0) + FACES * E == code[f : f + 1, :]))
        for t in range(2):
            at = (4 * t + f) * PITCH
            gath[at : at + 256, :] = gath[at : at + 256, :] + got[:, t * LANES : (t + 1) * LANES]

    def gathered(r):
        return gath[pl.ds(r, 8, stride=PITCH), :]

    def per_face(i):
        return jnp.concatenate(
            [jnp.broadcast_to(mat_v[i : i + 1, t * LANES : (t + 1) * LANES], (4, LANES)) for t in range(2)],
            axis=0,
        )

    kind8, turn8 = halves(kind), halves(turn)
    l1, g1, w1 = per_face(0), per_face(1), per_face(2)
    l2, g2, w2 = [gathered(NQ * FQ + i) + gathered(NQ * FQ + 3 + i) for i in range(3)]
    fastest = 0.5 * jnp.maximum(jnp.sqrt((l1 + 2.0 * g1) * w1), jnp.sqrt((l2 + 2.0 * g2) * w2))
    sign_v = jnp.where(kind8 == 3, 0.0, 1.0)
    sign_s = jnp.where(kind8 == 2, -1.0, sign_v)
    l1, g1, w1 = 0.5 * l1, 0.5 * g1, 0.5 * w1
    l2, g2, w2 = 0.5 * l2 * sign_v, 0.5 * g2 * sign_v, 0.5 * w2 * sign_s
    turn_one, turn_two = turn8 == 1, turn8 == 2

    @pl.loop(0, FQ // 3)
    def _(i):
        q0 = 3 * i
        outer = [[], [], []]
        for m in range(NQ):
            g = [gathered(m * FQ + q0 + k) for k in range(3)]
            for k in range(3):
                outer[k].append(
                    jnp.where(turn_one, g[(k + 1) % 3], jnp.where(turn_two, g[(k + 2) % 3], g[k]))
                )
        for k in range(3):
            q = q0 + k
            o = outer[k]
            u = [own[q, :, m * LANES : (m + 1) * LANES] for m in range(NQ)]
            n = [halves(nrm_v[j, q].astype(F32)) for j in range(3)]
            penalty = fastest * halves(ar_v[q])
            rigid = [g1 * u[6 + j] + g2 * o[6 + j] for j in range(3)]
            lame = [l1 * u[6 + j] + l2 * o[6 + j] for j in range(3)]
            stress = [w1 * u[s] + w2 * o[s] for s in range(6)]
            pressure = n[0] * lame[0] + n[1] * lame[1] + n[2] * lame[2]
            flux = [
                pressure + 2.0 * (n[0] * rigid[0]),
                pressure + 2.0 * (n[1] * rigid[1]),
                pressure + 2.0 * (n[2] * rigid[2]),
                n[0] * rigid[1] + n[1] * rigid[0],
                n[1] * rigid[2] + n[2] * rigid[1],
                n[0] * rigid[2] + n[2] * rigid[0],
                stress[0] * n[0] + stress[3] * n[1] + stress[5] * n[2],
                stress[3] * n[0] + stress[1] * n[1] + stress[4] * n[2],
                stress[5] * n[0] + stress[4] * n[1] + stress[2] * n[2],
            ]
            for m in range(NQ):
                sign = sign_s if m < 6 else sign_v
                flx[q, :, m * LANES : (m + 1) * LANES] = penalty * (u[m] - sign * o[m]) - flux[m]

    surface = mm(lift, flx[...].reshape(8 * FQ, WIDE).astype(BF16))

    @pl.loop(0, 16)
    def _(o):
        src = chip_at(o, -1)
        for a in range(2):
            metric_copy(2 * src + a, 2 * src + a).wait_recv()
        at = pl.multiple_of(16 * src, 16)
        u = [pts[pl.ds(at, 16), m * LANES : (m + 1) * LANES] for m in range(NQ)]
        for d in range(3):
            n = [
                jnp.concatenate(
                    [got8(recv, 2 * src, 3 * d + j), got8(recv, 2 * src + 1, 3 * d + j)], axis=0
                )
                for j in range(3)
            ]
            product = [
                n[0] * u[6],
                n[1] * u[7],
                n[2] * u[8],
                n[0] * u[7] + n[1] * u[6],
                n[1] * u[8] + n[2] * u[7],
                n[0] * u[8] + n[2] * u[6],
                u[0] * n[0] + u[3] * n[1] + u[5] * n[2],
                u[3] * n[0] + u[1] * n[1] + u[4] * n[2],
                u[5] * n[0] + u[4] * n[1] + u[2] * n[2],
            ]
            for m in range(NQ):
                fx[pl.ds(pl.multiple_of(d * 256 + at, 16), 16), m * LANES : (m + 1) * LANES] = product[
                    m
                ].astype(BF16)

    volume = mm(vgm[...], fx[...])
    for t in range(2):
        rows = slice(t * BP, (t + 1) * BP)
        lanes = slice(t * LANES, (t + 1) * LANES)
        v = [volume[rows, m * LANES : (m + 1) * LANES] for m in range(NQ)]
        l, g, w, step = [mat_v[i : i + 1, lanes] for i in range(4)]
        pressure = l * (v[0] + v[1] + v[2])
        for m in range(NQ):
            if m < 3:
                total = -(pressure + 2.0 * g * v[m])
            elif m < 6:
                total = -g * v[m]
            else:
                total = -w * v[m]
            total = total - surface[rows, m * LANES : (m + 1) * LANES]
            out[m, :, lanes] = st_v[m, :, lanes] + (step * total)[0:NB]

    @pl.loop(1, ROWS)
    def _(d):
        to = lax.rem(row + d, ROWS)
        metric_copy(to, row).wait_send()

    @pl.loop(1, COLS)
    def _(d):
        to = lax.rem(col + d, COLS)
        trace_copy(to, col).wait_send()


def got8(recv, r, k):
    return recv[r, k].astype(F32).reshape(8, LANES)


def per_device(
    state, geometry, material, neighbours, send_faces, vol_eval, vol_grad, face_eval, face_lift,
    normals, areas,
):
    geometry = jnp.transpose(geometry.reshape(9, 4, 2 * ROWS, LANES), (0, 2, 1, 3))
    face_eval = jnp.transpose(face_eval, (2, 0, 1))
    face_lift = jnp.transpose(face_lift, (2, 0, 1))
    args = (
        state, geometry, material, neighbours, send_faces, vol_eval, vol_grad, face_eval, face_lift,
        normals, areas,
    )
    staged = [a for i, a in enumerate(args) if i != 1]
    dma = pltpu.SemaphoreType.DMA
    return pl.pallas_call(
        kernel,
        out_shape=jax.ShapeDtypeStruct((NQ, NB, E), F32),
        in_specs=[pl.BlockSpec(memory_space=pl.ANY)] * len(args),
        out_specs=pl.BlockSpec(memory_space=pltpu.VMEM),
        scratch_shapes=[pltpu.VMEM(a.shape, a.dtype) for a in staged]
        + [
            pltpu.VMEM((ROWS, 9, 2, 4, LANES), BF16),
            pltpu.VMEM((COLS, SLOTS, 256), BF16),
            pltpu.VMEM((COLS, SLOTS, 256), BF16),
            pltpu.VMEM((KP, E), F32),
            pltpu.VMEM((2 * BP, WIDE), BF16),
            pltpu.VMEM((2, 8 * FQ, BP), F32),
            pltpu.VMEM((COLS * SLOTS, FACES * E), BF16),
            pltpu.VMEM((256, FACES * E), BF16),
            pltpu.VMEM((256, WIDE), F32),
            pltpu.VMEM((FQ, 8, WIDE), F32),
            pltpu.VMEM((8 * PITCH, LANES), F32),
            pltpu.VMEM((FQ, 8, WIDE), F32),
            pltpu.VMEM((3 * 256, WIDE), BF16),
            pltpu.VMEM((2 * BP, 3 * 256), BF16),
            dma((len(staged),)), dma((ROWS,)), dma((ROWS,)), dma((COLS,)), dma((COLS,)),
        ],
        compiler_params=pltpu.CompilerParams(
            collective_id=0, has_side_effects=True, vmem_limit_bytes=60 * 1024 * 1024
        ),
        name="section",
    )(*args)


def solution(mesh):
    blocks = P(None, None, ("col", "row"))
    in_specs = (
        blocks, P(None, "row", "col"), P(None, ("col", "row")), blocks, P(("col", "row"), None, None),
        P(), P(), P(), P(), P(None, None, None, ("col", "row")), blocks,
    )
    return jax.shard_map(
        per_device, mesh=mesh, in_specs=in_specs, out_specs=blocks, check_vma=False
    )
```

```python
import jax
import jax.numpy as jnp
from jax import lax
from jax.experimental import pallas as pl
from jax.experimental.pallas import tpu as pltpu
from jax.sharding import PartitionSpec as P

MESH = pl.DeviceIdType.MESH
F32, BF16, I32 = jnp.float32, jnp.bfloat16, jnp.int32

NQ, NB, BP = 9, 35, 40
FQ, FACES, E = 27, 4, 256
ROWS, COLS, SLOTS = 32, 8, 64
CHIPS = ROWS // 2
LANES = 128
WIDE = NQ * LANES
KP = NQ * BP + 8
PITCH = 264


def iota(shape, dim):
    return lax.broadcasted_iota(I32, shape, dim)


def ones_where(mask):
    return jnp.where(mask, 1.0, 0.0).astype(BF16)


def mm(a, b):
    return jnp.dot(a, b, preferred_element_type=F32)


def mm_t(a, b):
    return lax.dot_general(a, b, (((1,), (1,)), ((), ())), preferred_element_type=F32)


def halves(x):
    return jnp.concatenate([x[:, :LANES], x[:, LANES:]], axis=0)


def steps(x, size, count):
    result = jnp.zeros_like(x)
    for k in range(1, count):
        result = result + jnp.where(x >= size * k, 1, 0)
    return result


def kernel(
    state, geometry, material, neighbours, send_faces, vol_eval, vol_grad, face_eval, face_lift,
    normals, areas, out,
    st_v, mat_v, nb_v, sf_v, ve_v, vg_v, fe_v, fl_v, nrm_v, ar_v,
    recv, sendb, xr, sp, sb, raw, ohs, tr, pts, own, gath, flx, fx, vgm,
    load_sem, gsend_sem, grecv_sem, tsend_sem, trecv_sem, ready_sem,
):
    row, col = lax.axis_index("row"), lax.axis_index("col")
    chip, core = row // 2, row % 2
    cx, cy = chip // 4, chip % 4

    pairs = [
        (state, st_v), (material, mat_v), (neighbours, nb_v), (send_faces, sf_v), (vol_eval, ve_v),
        (vol_grad, vg_v), (face_eval, fe_v), (face_lift, fl_v), (normals, nrm_v), (areas, ar_v),
    ]
    loads = [pltpu.make_async_copy(a, b, load_sem.at[i]) for i, (a, b) in enumerate(pairs)]
    for copy in loads:
        copy.start()

    def block(p):
        return geometry.at[:, pl.ds(2 * p, 2)]

    local = pltpu.make_async_copy(block(row), recv.at[row], grecv_sem.at[row])
    local.start()

    barrier = pltpu.get_barrier_semaphore()

    def signal(sem, r, c):
        pl.semaphore_signal(sem, inc=1, device_id={"row": r, "col": c}, device_id_type=MESH)

    @pl.loop(1, COLS)
    def _(d):
        signal(barrier, 2 * chip, lax.rem(col + d, COLS))

    @pl.loop(1, CHIPS)
    def _(d):
        signal(barrier, 2 * lax.rem(chip + d, CHIPS) + 1, col)

    signal(barrier, 2 * chip + (1 - core), col)

    def metric_copy(to, source):
        return pltpu.make_async_remote_copy(
            src_ref=block(to), dst_ref=recv.at[source], send_sem=gsend_sem.at[to],
            recv_sem=grecv_sem.at[source], device_id={"row": to, "col": col}, device_id_type=MESH,
        )

    def trace_copy(to, source):
        return pltpu.make_async_remote_copy(
            src_ref=sendb.at[to], dst_ref=xr.at[source], send_sem=tsend_sem.at[to],
            recv_sem=trecv_sem.at[source], device_id={"row": row, "col": to}, device_id_type=MESH,
        )

    def chip_at(o, sign):
        dx, dy = o // 4, o % 4
        return lax.rem(cx + sign * dx + 4, 4) * 4 + lax.rem(cy + sign * dy + 4, 4)

    for copy in loads:
        copy.wait()
    for m in range(NQ):
        sp[m * BP : m * BP + NB, :] = st_v[m]
        sp[m * BP + NB : (m + 1) * BP, :] = jnp.zeros((BP - NB, E), F32)
    high = mat_v[0:3, :].astype(BF16).astype(F32)
    sp[NQ * BP : NQ * BP + 3, :] = high
    sp[NQ * BP + 3 : NQ * BP + 6, :] = mat_v[0:3, :] - high
    sp[NQ * BP + 6 : KP, :] = jnp.zeros((2, E), F32)
    dof = sp[...].astype(BF16)

    raw[...] = jnp.zeros(raw.shape, F32)
    for q in range(FQ):
        for t in range(2):
            raw[0, 8 * q + 4 * t : 8 * q + 4 * t + 4, 0:NB] = fe_v[q]
            raw[1, 8 * q + 4 * t : 8 * q + 4 * t + 4, 0:NB] = fl_v[q]
    eval_rows = raw[0].astype(BF16)
    lift_rows = raw[1].astype(BF16)

    col_kp = iota((1, KP), 1)
    m_col = steps(col_kp, BP, NQ)
    spread9 = ones_where((iota((BP, 1), 0) == col_kp - BP * m_col) & (col_kp < NQ * BP))
    wide_eval = mm(eval_rows, spread9).astype(BF16)
    row_t = iota((256, 1), 0)
    m_row = steps(row_t, FQ, NQ)
    q_row = row_t - FQ * m_row
    same = (m_row == m_col) & (row_t < NQ * FQ) & (col_kp < NQ * BP)
    carry = (row_t - NQ * FQ == col_kp - NQ * BP) & (col_kp >= NQ * BP)
    for f in range(FACES):
        pick = ones_where(iota((1, 8 * FQ), 1) == 8 * q_row + f)
        weights = jnp.where(same, mm(pick, wide_eval), jnp.where(carry, 1.0, 0.0)).astype(BF16)
        tr[:, f * E : (f + 1) * E] = mm(weights, dof).astype(BF16)

    listed = jnp.transpose(jnp.concatenate([sf_v[0], sf_v[0]], axis=1))
    for p in range(COLS):
        ohs[p * SLOTS : (p + 1) * SLOTS, :] = ones_where(
            listed[0:SLOTS, p : p + 1] == iota((1, FACES * E), 1)
        )
    outgoing = mm_t(ohs[...], tr[...]).astype(BF16)
    for p in range(COLS):
        sendb[p] = outgoing[p * SLOTS : (p + 1) * SLOTS, :]
    xr[col] = jnp.zeros((SLOTS, 256), BF16)

    @pl.when(core == 0)
    def _():
        pl.semaphore_wait(barrier, 2 * (COLS - 1) + 1)
        signal(ready_sem, row + 1, col)

    @pl.when(core == 1)
    def _():
        pl.semaphore_wait(ready_sem, 1)

    @pl.loop(1, COLS)
    def _(d):
        trace_copy(lax.rem(col + d, COLS), col).start()

    @pl.when(core == 1)
    def _():
        pl.semaphore_wait(barrier, ROWS - 1)
        signal(ready_sem, row - 1, col)

    @pl.when(core == 0)
    def _():
        pl.semaphore_wait(ready_sem, 1)

    metric_copy(2 * chip + (1 - core), row).start()

    @pl.loop(1, CHIPS)
    def _(o):
        peer = chip_at(o, 1)
        metric_copy(2 * peer + core, row).start()
        metric_copy(2 * peer + (1 - core), row).start()

    for m in range(NQ):
        both = jnp.concatenate(
            [sp[m * BP : (m + 1) * BP, :LANES], sp[m * BP : (m + 1) * BP, LANES:]], axis=0
        )
        sb[:, m * LANES : (m + 1) * LANES] = both.astype(BF16)
    tile_col = jnp.where(iota((1, 2 * BP), 1) >= BP, 1, 0)
    twice = ones_where(iota((BP, 1), 0) == iota((1, 2 * BP), 1) - BP * tile_col)
    face_row = iota((8 * FQ, 1), 0)
    eval_mask = ((face_row >> 2) & 1) == tile_col
    face_weights = jnp.where(eval_mask, mm(eval_rows, twice), 0.0).astype(BF16)
    own[...] = mm(face_weights, sb[...]).reshape(FQ, 8, WIDE)
    point_row = iota((256, 1), 0)
    spread_v = ones_where(iota((1, 128), 1) == 4 * (point_row >> 3) + (point_row & 3))
    pad = jnp.zeros((BP - NB, 128), F32)
    eval2 = jnp.concatenate([ve_v[...], pad, ve_v[...], pad], axis=0).astype(BF16)
    vol_mask = ((point_row >> 2) & 1) == tile_col
    vol_weights = jnp.where(vol_mask, mm_t(spread_v, eval2), 0.0).astype(BF16)
    pts[...] = mm(vol_weights, sb[...])
    tile_row = jnp.where(iota((2 * BP, 1), 0) >= BP, 1, 0)
    grad_mask = tile_row == ((iota((1, 256), 1) >> 2) & 1)
    for d in range(3):
        grad = vg_v[d].astype(F32)
        grad2 = jnp.concatenate([grad, pad, grad, pad], axis=0).astype(BF16)
        vgm[:, d * 256 : (d + 1) * 256] = jnp.where(grad_mask, mm_t(grad2, spread_v), 0.0).astype(BF16)
    twice_t = ones_where(iota((2 * BP, 1), 0) - BP * tile_row == iota((1, BP), 1))
    lift_mask = tile_row == ((iota((1, 8 * FQ), 1) >> 2) & 1)
    lift = jnp.where(lift_mask, mm_t(twice_t, lift_rows), 0.0).astype(BF16)

    kind, peer, target, turn = nb_v[0], nb_v[1], nb_v[2], nb_v[3]
    face_id = iota((FACES, E), 0) * E + iota((FACES, E), 1)
    code = jnp.where(
        kind == 0, target, jnp.where(kind == 1, FACES * E + peer * SLOTS + target, face_id)
    )
    for f in range(FACES):
        got = mm(tr[...], ones_where(iota((FACES * E, 1), 0) == code[f : f + 1, :]))
        for t in range(2):
            gath[(4 * t + f) * PITCH : (4 * t + f) * PITCH + 256, :] = got[:, t * LANES : (t + 1) * LANES]

    @pl.loop(1, COLS)
    def _(d):
        source = lax.rem(col + COLS - d, COLS)
        trace_copy(source, source).wait_recv()

    ident = ones_where(iota((256, 1), 0) == iota((1, 256), 1))
    xt = mm_t(ident, xr[...].reshape(COLS * SLOTS, 256)).astype(BF16)
    for f in range(FACES):
        got = mm(xt, ones_where(iota((COLS * SLOTS, 1), 0) + FACES * E == code[f : f + 1, :]))
        for t in range(2):
            at = (4 * t + f) * PITCH
            gath[at : at + 256, :] = gath[at : at + 256, :] + got[:, t * LANES : (t + 1) * LANES]

    def gathered(r):
        return gath[pl.ds(r, 8, stride=PITCH), :]

    def per_face(i):
        return jnp.concatenate(
            [jnp.broadcast_to(mat_v[i : i + 1, t * LANES : (t + 1) * LANES], (4, LANES)) for t in range(2)],
            axis=0,
        )

    kind8, turn8 = halves(kind), halves(turn)
    l1, g1, w1 = per_face(0), per_face(1), per_face(2)
    l2, g2, w2 = [gathered(NQ * FQ + i) + gathered(NQ * FQ + 3 + i) for i in range(3)]
    fastest = 0.5 * jnp.maximum(jnp.sqrt((l1 + 2.0 * g1) * w1), jnp.sqrt((l2 + 2.0 * g2) * w2))
    sign_v = jnp.where(kind8 == 3, 0.0, 1.0)
    sign_s = jnp.where(kind8 == 2, -1.0, sign_v)
    l1, g1, w1 = 0.5 * l1, 0.5 * g1, 0.5 * w1
    l2, g2, w2 = 0.5 * l2 * sign_v, 0.5 * g2 * sign_v, 0.5 * w2 * sign_s
    turn_one, turn_two = turn8 == 1, turn8 == 2

    @pl.loop(0, FQ // 3)
    def _(i):
        q0 = 3 * i
        outer = [[], [], []]
        for m in range(NQ):
            g = [gathered(m * FQ + q0 + k) for k in range(3)]
            for k in range(3):
                outer[k].append(
                    jnp.where(turn_one, g[(k + 1) % 3], jnp.where(turn_two, g[(k + 2) % 3], g[k]))
                )
        for k in range(3):
            q = q0 + k
            o = outer[k]
            u = [own[q, :, m * LANES : (m + 1) * LANES] for m in range(NQ)]
            n = [halves(nrm_v[j, q].astype(F32)) for j in range(3)]
            penalty = fastest * halves(ar_v[q])
            rigid = [g1 * u[6 + j] + g2 * o[6 + j] for j in range(3)]
            lame = [l1 * u[6 + j] + l2 * o[6 + j] for j in range(3)]
            stress = [w1 * u[s] + w2 * o[s] for s in range(6)]
            pressure = n[0] * lame[0] + n[1] * lame[1] + n[2] * lame[2]
            flux = [
                pressure + 2.0 * (n[0] * rigid[0]),
                pressure + 2.0 * (n[1] * rigid[1]),
                pressure + 2.0 * (n[2] * rigid[2]),
                n[0] * rigid[1] + n[1] * rigid[0],
                n[1] * rigid[2] + n[2] * rigid[1],
                n[0] * rigid[2] + n[2] * rigid[0],
                stress[0] * n[0] + stress[3] * n[1] + stress[5] * n[2],
                stress[3] * n[0] + stress[1] * n[1] + stress[4] * n[2],
                stress[5] * n[0] + stress[4] * n[1] + stress[2] * n[2],
            ]
            for m in range(NQ):
                sign = sign_s if m < 6 else sign_v
                flx[q, :, m * LANES : (m + 1) * LANES] = penalty * (u[m] - sign * o[m]) - flux[m]

    surface = mm(lift, flx[...].reshape(8 * FQ, WIDE).astype(BF16))

    @pl.loop(0, CHIPS)
    def _(o):
        src = chip_at(o, -1)
        for a in range(2):
            metric_copy(2 * src + a, 2 * src + a).wait_recv()
        at = pl.multiple_of(16 * src, 16)
        u = [pts[pl.ds(at, 16), m * LANES : (m + 1) * LANES] for m in range(NQ)]
        for d in range(3):
            n = [
                jnp.concatenate(
                    [got8(recv, 2 * src, 3 * d + j), got8(recv, 2 * src + 1, 3 * d + j)], axis=0
                )
                for j in range(3)
            ]
            product = [
                n[0] * u[6],
                n[1] * u[7],
                n[2] * u[8],
                n[0] * u[7] + n[1] * u[6],
                n[1] * u[8] + n[2] * u[7],
                n[0] * u[8] + n[2] * u[6],
                u[0] * n[0] + u[3] * n[1] + u[5] * n[2],
                u[3] * n[0] + u[1] * n[1] + u[4] * n[2],
                u[5] * n[0] + u[4] * n[1] + u[2] * n[2],
            ]
            for m in range(NQ):
                fx[pl.ds(pl.multiple_of(d * 256 + at, 16), 16), m * LANES : (m + 1) * LANES] = product[
                    m
                ].astype(BF16)

    volume = mm(vgm[...], fx[...])
    for t in range(2):
        rows = slice(t * BP, (t + 1) * BP)
        lanes = slice(t * LANES, (t + 1) * LANES)
        v = [volume[rows, m * LANES : (m + 1) * LANES] for m in range(NQ)]
        l, g, w, step = [mat_v[i : i + 1, lanes] for i in range(4)]
        pressure = l * (v[0] + v[1] + v[2])
        for m in range(NQ):
            if m < 3:
                total = -(pressure + 2.0 * g * v[m])
            elif m < 6:
                total = -g * v[m]
            else:
                total = -w * v[m]
            total = total - surface[rows, m * LANES : (m + 1) * LANES]
            out[m, :, lanes] = st_v[m, :, lanes] + (step * total)[0:NB]

    @pl.loop(1, ROWS)
    def _(d):
        to = lax.rem(row + d, ROWS)
        metric_copy(to, row).wait_send()

    @pl.loop(1, COLS)
    def _(d):
        to = lax.rem(col + d, COLS)
        trace_copy(to, col).wait_send()


def got8(recv, r, k):
    return recv[r, k].astype(F32).reshape(8, LANES)


def per_device(
    state, geometry, material, neighbours, send_faces, vol_eval, vol_grad, face_eval, face_lift,
    normals, areas,
):
    geometry = jnp.transpose(geometry.reshape(9, 4, 2 * ROWS, LANES), (0, 2, 1, 3))
    face_eval = jnp.transpose(face_eval, (2, 0, 1))
    face_lift = jnp.transpose(face_lift, (2, 0, 1))
    args = (
        state, geometry, material, neighbours, send_faces, vol_eval, vol_grad, face_eval, face_lift,
        normals, areas,
    )
    args = tuple(pltpu.with_memory_space_constraint(a, pltpu.HBM) for a in args)
    staged = [a for i, a in enumerate(args) if i != 1]
    dma = pltpu.SemaphoreType.DMA
    return pl.pallas_call(
        kernel,
        out_shape=jax.ShapeDtypeStruct((NQ, NB, E), F32),
        in_specs=[pl.BlockSpec(memory_space=pl.ANY)] * len(args),
        out_specs=pl.BlockSpec(memory_space=pltpu.VMEM),
        scratch_shapes=[pltpu.VMEM(a.shape, a.dtype) for a in staged]
        + [
            pltpu.VMEM((ROWS, 9, 2, 4, LANES), BF16),
            pltpu.VMEM((COLS, SLOTS, 256), BF16),
            pltpu.VMEM((COLS, SLOTS, 256), BF16),
            pltpu.VMEM((KP, E), F32),
            pltpu.VMEM((2 * BP, WIDE), BF16),
            pltpu.VMEM((2, 8 * FQ, BP), F32),
            pltpu.VMEM((COLS * SLOTS, FACES * E), BF16),
            pltpu.VMEM((256, FACES * E), BF16),
            pltpu.VMEM((256, WIDE), F32),
            pltpu.VMEM((FQ, 8, WIDE), F32),
            pltpu.VMEM((8 * PITCH, LANES), F32),
            pltpu.VMEM((FQ, 8, WIDE), F32),
            pltpu.VMEM((3 * 256, WIDE), BF16),
            pltpu.VMEM((2 * BP, 3 * 256), BF16),
            dma((len(staged),)), dma((ROWS,)), dma((ROWS,)), dma((COLS,)), dma((COLS,)),
            pltpu.SemaphoreType.REGULAR,
        ],
        compiler_params=pltpu.CompilerParams(
            collective_id=0, has_side_effects=True, vmem_limit_bytes=40 * 1024 * 1024
        ),
        name="section",
    )(*args)


def solution(mesh):
    blocks = P(None, None, ("col", "row"))
    in_specs = (
        blocks, P(None, "row", "col"), P(None, ("col", "row")), blocks, P(("col", "row"), None, None),
        P(), P(), P(), P(), P(None, None, None, ("col", "row")), blocks,
    )
    return jax.shard_map(
        per_device, mesh=mesh, in_specs=in_specs, out_specs=blocks, check_vma=False
    )
```

```python
import jax
import jax.numpy as jnp
from jax import lax
from jax.experimental import pallas as pl
from jax.experimental.pallas import tpu as pltpu
from jax.sharding import PartitionSpec as P

MESH = pl.DeviceIdType.MESH
F32, BF16, I32 = jnp.float32, jnp.bfloat16, jnp.int32

NQ, NB, BP = 9, 35, 40
FQ, FACES, E = 27, 4, 256
ROWS, COLS, SLOTS = 32, 8, 64
CHIPS = ROWS // 2
EARLY = 4
FAR = ((2, 2), (2, 1), (1, 2), (2, 3), (3, 2), (2, 0), (0, 2), (1, 1), (3, 3), (1, 3), (3, 1), (1, 0), (0, 1), (3, 0), (0, 3), (0, 0))
LANES = 128
WIDE = NQ * LANES
KP = NQ * BP + 8
PITCH = 264


def iota(shape, dim):
    return lax.broadcasted_iota(I32, shape, dim)


def ones_where(mask):
    return jnp.where(mask, 1.0, 0.0).astype(BF16)


def mm(a, b):
    return jnp.dot(a, b, preferred_element_type=F32)


def mm_t(a, b):
    return lax.dot_general(a, b, (((1,), (1,)), ((), ())), preferred_element_type=F32)


def halves(x):
    return jnp.concatenate([x[:, :LANES], x[:, LANES:]], axis=0)


def steps(x, size, count):
    result = jnp.zeros_like(x)
    for k in range(1, count):
        result = result + jnp.where(x >= size * k, 1, 0)
    return result


def face_rows(source, raw):
    raw[...] = jnp.zeros(raw.shape, F32)
    for q in range(FQ):
        for t in range(2):
            raw[8 * q + 4 * t : 8 * q + 4 * t + 4, 0:NB] = source[q]
    return raw[...].astype(BF16)


def kernel(
    state, geometry, material, neighbours, send_faces, vol_eval, vol_grad, face_eval, face_lift,
    normals, areas, out,
    st_v, mat_v, nb_v, sf_v, ve_v, vg_v, fe_v, fl_v, nrm_v, ar_v,
    recv, sendb, xr, sp, sb, raw, ohs, tr, pts, own, gath, flx, fx, vgm,
    load_sem, gsend_sem, grecv_sem, tsend_sem, trecv_sem, ready_sem,
):
    row, col = lax.axis_index("row"), lax.axis_index("col")
    chip, core = row // 2, row % 2
    cx, cy = chip // 4, chip % 4

    pairs = [
        (state, st_v), (material, mat_v), (neighbours, nb_v), (send_faces, sf_v), (vol_eval, ve_v),
        (vol_grad, vg_v), (face_eval, fe_v), (face_lift, fl_v), (normals, nrm_v), (areas, ar_v),
    ]
    loads = [pltpu.make_async_copy(a, b, load_sem.at[i]) for i, (a, b) in enumerate(pairs)]
    for copy in loads:
        copy.start()

    def block(p):
        return geometry.at[:, pl.ds(2 * p, 2)]

    local = pltpu.make_async_copy(block(row), recv.at[row], grecv_sem.at[row])
    local.start()

    barrier = pltpu.get_barrier_semaphore()

    def signal(sem, r, c):
        pl.semaphore_signal(sem, inc=1, device_id={"row": r, "col": c}, device_id_type=MESH)

    @pl.loop(1, COLS)
    def _(d):
        signal(barrier, 2 * chip, lax.rem(col + d, COLS))

    @pl.loop(1, CHIPS)
    def _(d):
        signal(barrier, 2 * lax.rem(chip + d, CHIPS) + 1, col)

    signal(barrier, 2 * chip + (1 - core), col)

    def metric_copy(to, source):
        return pltpu.make_async_remote_copy(
            src_ref=block(to), dst_ref=recv.at[source], send_sem=gsend_sem.at[to],
            recv_sem=grecv_sem.at[source], device_id={"row": to, "col": col}, device_id_type=MESH,
        )

    def trace_copy(to, source):
        return pltpu.make_async_remote_copy(
            src_ref=sendb.at[to], dst_ref=xr.at[source], send_sem=tsend_sem.at[to],
            recv_sem=trecv_sem.at[source], device_id={"row": row, "col": to}, device_id_type=MESH,
        )

    def chip_at(o, sign):
        dx, dy = o // 4, o % 4
        return lax.rem(cx + sign * dx + 4, 4) * 4 + lax.rem(cy + sign * dy + 4, 4)

    for i in (0, 1, 3, 6):
        loads[i].wait()
    for m in range(NQ):
        sp[m * BP : m * BP + NB, :] = st_v[m]
        sp[m * BP + NB : (m + 1) * BP, :] = jnp.zeros((BP - NB, E), F32)
    high = mat_v[0:3, :].astype(BF16).astype(F32)
    sp[NQ * BP : NQ * BP + 3, :] = high
    sp[NQ * BP + 3 : NQ * BP + 6, :] = mat_v[0:3, :] - high
    sp[NQ * BP + 6 : KP, :] = jnp.zeros((2, E), F32)
    dof = sp[...].astype(BF16)

    eval_rows = face_rows(fe_v, raw.at[0])

    col_kp = iota((1, KP), 1)
    m_col = steps(col_kp, BP, NQ)
    spread9 = ones_where((iota((BP, 1), 0) == col_kp - BP * m_col) & (col_kp < NQ * BP))
    wide_eval = mm(eval_rows, spread9).astype(BF16)
    row_t = iota((256, 1), 0)
    m_row = steps(row_t, FQ, NQ)
    q_row = row_t - FQ * m_row
    same = (m_row == m_col) & (row_t < NQ * FQ) & (col_kp < NQ * BP)
    carry = (row_t - NQ * FQ == col_kp - NQ * BP) & (col_kp >= NQ * BP)
    for f in range(FACES):
        pick = ones_where(iota((1, 8 * FQ), 1) == 8 * q_row + f)
        weights = jnp.where(same, mm(pick, wide_eval), jnp.where(carry, 1.0, 0.0)).astype(BF16)
        tr[:, f * E : (f + 1) * E] = mm(weights, dof).astype(BF16)

    listed = jnp.transpose(jnp.concatenate([sf_v[0], sf_v[0]], axis=1))
    for p in range(COLS):
        ohs[p * SLOTS : (p + 1) * SLOTS, :] = ones_where(
            listed[0:SLOTS, p : p + 1] == iota((1, FACES * E), 1)
        )
    outgoing = mm_t(ohs[...], tr[...]).astype(BF16)
    for p in range(COLS):
        sendb[p] = outgoing[p * SLOTS : (p + 1) * SLOTS, :]
    xr[col] = jnp.zeros((SLOTS, 256), BF16)

    def wait_column():
        @pl.when(core == 0)
        def _():
            pl.semaphore_wait(barrier, 2 * (COLS - 1) + 1)
            signal(ready_sem, row + 1, col)

        @pl.when(core == 1)
        def _():
            pl.semaphore_wait(ready_sem, 1)

    def wait_plane():
        @pl.when(core == 1)
        def _():
            pl.semaphore_wait(barrier, ROWS - 1)
            signal(ready_sem, row - 1, col)

        @pl.when(core == 0)
        def _():
            pl.semaphore_wait(ready_sem, 1)

    def send_traces():
        @pl.loop(0, COLS - 1)
        def _(i):
            trace_copy(i + jnp.where(i >= col, 1, 0), col).start()

    def send_metric():
        for dx, dy in FAR:
            peer = lax.rem(cx + dx, 4) * 4 + lax.rem(cy + dy, 4)
            if (dx, dy) != (0, 0):
                metric_copy(2 * peer + core, row).start()
            metric_copy(2 * peer + (1 - core), row).start()

    @pl.when(col >= EARLY)
    def _():
        wait_column()
        send_traces()
        wait_plane()
        send_metric()

    @pl.when(col < EARLY)
    def _():
        wait_plane()
        send_metric()
        wait_column()
        send_traces()

    for i in (2, 4, 5, 7, 8, 9):
        loads[i].wait()

    for m in range(NQ):
        both = jnp.concatenate(
            [sp[m * BP : (m + 1) * BP, :LANES], sp[m * BP : (m + 1) * BP, LANES:]], axis=0
        )
        sb[:, m * LANES : (m + 1) * LANES] = both.astype(BF16)
    tile_col = jnp.where(iota((1, 2 * BP), 1) >= BP, 1, 0)
    twice = ones_where(iota((BP, 1), 0) == iota((1, 2 * BP), 1) - BP * tile_col)
    face_row = iota((8 * FQ, 1), 0)
    eval_mask = ((face_row >> 2) & 1) == tile_col
    face_weights = jnp.where(eval_mask, mm(eval_rows, twice), 0.0).astype(BF16)
    own[...] = mm(face_weights, sb[...]).reshape(FQ, 8, WIDE)
    point_row = iota((256, 1), 0)
    spread_v = ones_where(iota((1, 128), 1) == 4 * (point_row >> 3) + (point_row & 3))
    pad = jnp.zeros((BP - NB, 128), F32)
    eval2 = jnp.concatenate([ve_v[...], pad, ve_v[...], pad], axis=0).astype(BF16)
    vol_mask = ((point_row >> 2) & 1) == tile_col
    vol_weights = jnp.where(vol_mask, mm_t(spread_v, eval2), 0.0).astype(BF16)
    pts[...] = mm(vol_weights, sb[...])
    tile_row = jnp.where(iota((2 * BP, 1), 0) >= BP, 1, 0)
    grad_mask = tile_row == ((iota((1, 256), 1) >> 2) & 1)
    for d in range(3):
        grad = vg_v[d].astype(F32)
        grad2 = jnp.concatenate([grad, pad, grad, pad], axis=0).astype(BF16)
        vgm[:, d * 256 : (d + 1) * 256] = jnp.where(grad_mask, mm_t(grad2, spread_v), 0.0).astype(BF16)
    twice_t = ones_where(iota((2 * BP, 1), 0) - BP * tile_row == iota((1, BP), 1))
    lift_mask = tile_row == ((iota((1, 8 * FQ), 1) >> 2) & 1)
    lift_rows = face_rows(fl_v, raw.at[1])
    lift = jnp.where(lift_mask, mm_t(twice_t, lift_rows), 0.0).astype(BF16)

    kind, peer, target, turn = nb_v[0], nb_v[1], nb_v[2], nb_v[3]
    face_id = iota((FACES, E), 0) * E + iota((FACES, E), 1)
    code = jnp.where(
        kind == 0, target, jnp.where(kind == 1, FACES * E + peer * SLOTS + target, face_id)
    )
    for f in range(FACES):
        got = mm(tr[...], ones_where(iota((FACES * E, 1), 0) == code[f : f + 1, :]))
        for t in range(2):
            gath[(4 * t + f) * PITCH : (4 * t + f) * PITCH + 256, :] = got[:, t * LANES : (t + 1) * LANES]

    @pl.loop(1, COLS)
    def _(d):
        source = lax.rem(col + COLS - d, COLS)
        trace_copy(source, source).wait_recv()

    ident = ones_where(iota((256, 1), 0) == iota((1, 256), 1))
    xt = mm_t(ident, xr[...].reshape(COLS * SLOTS, 256)).astype(BF16)
    for f in range(FACES):
        got = mm(xt, ones_where(iota((COLS * SLOTS, 1), 0) + FACES * E == code[f : f + 1, :]))
        for t in range(2):
            at = (4 * t + f) * PITCH
            gath[at : at + 256, :] = gath[at : at + 256, :] + got[:, t * LANES : (t + 1) * LANES]

    def gathered(r):
        return gath[pl.ds(r, 8, stride=PITCH), :]

    def per_face(i):
        return jnp.concatenate(
            [jnp.broadcast_to(mat_v[i : i + 1, t * LANES : (t + 1) * LANES], (4, LANES)) for t in range(2)],
            axis=0,
        )

    kind8, turn8 = halves(kind), halves(turn)
    l1, g1, w1 = per_face(0), per_face(1), per_face(2)
    l2, g2, w2 = [gathered(NQ * FQ + i) + gathered(NQ * FQ + 3 + i) for i in range(3)]
    fastest = 0.5 * jnp.maximum(jnp.sqrt((l1 + 2.0 * g1) * w1), jnp.sqrt((l2 + 2.0 * g2) * w2))
    sign_v = jnp.where(kind8 == 3, 0.0, 1.0)
    sign_s = jnp.where(kind8 == 2, -1.0, sign_v)
    l1, g1, w1 = 0.5 * l1, 0.5 * g1, 0.5 * w1
    l2, g2, w2 = 0.5 * l2 * sign_v, 0.5 * g2 * sign_v, 0.5 * w2 * sign_s
    turn_one, turn_two = turn8 == 1, turn8 == 2

    @pl.loop(0, FQ // 3)
    def _(i):
        q0 = 3 * i
        outer = [[], [], []]
        for m in range(NQ):
            g = [gathered(m * FQ + q0 + k) for k in range(3)]
            for k in range(3):
                outer[k].append(
                    jnp.where(turn_one, g[(k + 1) % 3], jnp.where(turn_two, g[(k + 2) % 3], g[k]))
                )
        for k in range(3):
            q = q0 + k
            o = outer[k]
            u = [own[q, :, m * LANES : (m + 1) * LANES] for m in range(NQ)]
            n = [halves(nrm_v[j, q].astype(F32)) for j in range(3)]
            penalty = fastest * halves(ar_v[q])
            rigid = [g1 * u[6 + j] + g2 * o[6 + j] for j in range(3)]
            lame = [l1 * u[6 + j] + l2 * o[6 + j] for j in range(3)]
            stress = [w1 * u[s] + w2 * o[s] for s in range(6)]
            pressure = n[0] * lame[0] + n[1] * lame[1] + n[2] * lame[2]
            flux = [
                pressure + 2.0 * (n[0] * rigid[0]),
                pressure + 2.0 * (n[1] * rigid[1]),
                pressure + 2.0 * (n[2] * rigid[2]),
                n[0] * rigid[1] + n[1] * rigid[0],
                n[1] * rigid[2] + n[2] * rigid[1],
                n[0] * rigid[2] + n[2] * rigid[0],
                stress[0] * n[0] + stress[3] * n[1] + stress[5] * n[2],
                stress[3] * n[0] + stress[1] * n[1] + stress[4] * n[2],
                stress[5] * n[0] + stress[4] * n[1] + stress[2] * n[2],
            ]
            for m in range(NQ):
                sign = sign_s if m < 6 else sign_v
                flx[q, :, m * LANES : (m + 1) * LANES] = penalty * (u[m] - sign * o[m]) - flux[m]

    surface = mm(lift, flx[...].reshape(8 * FQ, WIDE).astype(BF16))

    @pl.loop(0, CHIPS)
    def _(o):
        src = chip_at(o, -1)
        for a in range(2):
            metric_copy(2 * src + a, 2 * src + a).wait_recv()
        at = pl.multiple_of(16 * src, 16)
        u = [pts[pl.ds(at, 16), m * LANES : (m + 1) * LANES] for m in range(NQ)]
        for d in range(3):
            n = [
                jnp.concatenate(
                    [got8(recv, 2 * src, 3 * d + j), got8(recv, 2 * src + 1, 3 * d + j)], axis=0
                )
                for j in range(3)
            ]
            product = [
                n[0] * u[6],
                n[1] * u[7],
                n[2] * u[8],
                n[0] * u[7] + n[1] * u[6],
                n[1] * u[8] + n[2] * u[7],
                n[0] * u[8] + n[2] * u[6],
                u[0] * n[0] + u[3] * n[1] + u[5] * n[2],
                u[3] * n[0] + u[1] * n[1] + u[4] * n[2],
                u[5] * n[0] + u[4] * n[1] + u[2] * n[2],
            ]
            for m in range(NQ):
                fx[pl.ds(pl.multiple_of(d * 256 + at, 16), 16), m * LANES : (m + 1) * LANES] = product[
                    m
                ].astype(BF16)

    volume = mm(vgm[...], fx[...])
    for t in range(2):
        rows = slice(t * BP, (t + 1) * BP)
        lanes = slice(t * LANES, (t + 1) * LANES)
        v = [volume[rows, m * LANES : (m + 1) * LANES] for m in range(NQ)]
        l, g, w, step = [mat_v[i : i + 1, lanes] for i in range(4)]
        pressure = l * (v[0] + v[1] + v[2])
        for m in range(NQ):
            if m < 3:
                total = -(pressure + 2.0 * g * v[m])
            elif m < 6:
                total = -g * v[m]
            else:
                total = -w * v[m]
            total = total - surface[rows, m * LANES : (m + 1) * LANES]
            out[m, :, lanes] = st_v[m, :, lanes] + (step * total)[0:NB]

    @pl.loop(1, ROWS)
    def _(d):
        to = lax.rem(row + d, ROWS)
        metric_copy(to, row).wait_send()

    @pl.loop(1, COLS)
    def _(d):
        to = lax.rem(col + d, COLS)
        trace_copy(to, col).wait_send()


def got8(recv, r, k):
    return recv[r, k].astype(F32).reshape(8, LANES)


def per_device(
    state, geometry, material, neighbours, send_faces, vol_eval, vol_grad, face_eval, face_lift,
    normals, areas,
):
    geometry = jnp.transpose(geometry.reshape(9, 4, 2 * ROWS, LANES), (0, 2, 1, 3))
    face_eval = jnp.transpose(face_eval, (2, 0, 1))
    face_lift = jnp.transpose(face_lift, (2, 0, 1))
    args = (
        state, geometry, material, neighbours, send_faces, vol_eval, vol_grad, face_eval, face_lift,
        normals, areas,
    )
    args = tuple(pltpu.with_memory_space_constraint(a, pltpu.HBM) for a in args)
    staged = [a for i, a in enumerate(args) if i != 1]
    dma = pltpu.SemaphoreType.DMA
    return pl.pallas_call(
        kernel,
        out_shape=jax.ShapeDtypeStruct((NQ, NB, E), F32),
        in_specs=[pl.BlockSpec(memory_space=pl.ANY)] * len(args),
        out_specs=pl.BlockSpec(memory_space=pltpu.VMEM),
        scratch_shapes=[pltpu.VMEM(a.shape, a.dtype) for a in staged]
        + [
            pltpu.VMEM((ROWS, 9, 2, 4, LANES), BF16),
            pltpu.VMEM((COLS, SLOTS, 256), BF16),
            pltpu.VMEM((COLS, SLOTS, 256), BF16),
            pltpu.VMEM((KP, E), F32),
            pltpu.VMEM((2 * BP, WIDE), BF16),
            pltpu.VMEM((2, 8 * FQ, BP), F32),
            pltpu.VMEM((COLS * SLOTS, FACES * E), BF16),
            pltpu.VMEM((256, FACES * E), BF16),
            pltpu.VMEM((256, WIDE), F32),
            pltpu.VMEM((FQ, 8, WIDE), F32),
            pltpu.VMEM((8 * PITCH, LANES), F32),
            pltpu.VMEM((FQ, 8, WIDE), F32),
            pltpu.VMEM((3 * 256, WIDE), BF16),
            pltpu.VMEM((2 * BP, 3 * 256), BF16),
            dma((len(staged),)), dma((ROWS,)), dma((ROWS,)), dma((COLS,)), dma((COLS,)),
            pltpu.SemaphoreType.REGULAR,
        ],
        compiler_params=pltpu.CompilerParams(
            collective_id=0, has_side_effects=True, vmem_limit_bytes=40 * 1024 * 1024
        ),
        name="section",
    )(*args)


def solution(mesh):
    blocks = P(None, None, ("col", "row"))
    in_specs = (
        blocks, P(None, "row", "col"), P(None, ("col", "row")), blocks, P(("col", "row"), None, None),
        P(), P(), P(), P(), P(None, None, None, ("col", "row")), blocks,
    )
    return jax.shard_map(
        per_device, mesh=mesh, in_specs=in_specs, out_specs=blocks, check_vma=False
    )
```

```python
import jax
import jax.numpy as jnp
from jax import lax
from jax.experimental import pallas as pl
from jax.experimental.pallas import tpu as pltpu
from jax.sharding import PartitionSpec as P

MESH = pl.DeviceIdType.MESH
F32, BF16, I32 = jnp.float32, jnp.bfloat16, jnp.int32

NQ, NB, BP = 9, 35, 40
FQ, FACES, E = 27, 4, 256
ROWS, COLS, SLOTS = 32, 8, 64
CHIPS = ROWS // 2
EARLY = 4
FAR = ((2, 2), (2, 1), (1, 2), (2, 3), (3, 2), (2, 0), (0, 2), (1, 1), (3, 3), (1, 3), (3, 1), (1, 0), (0, 1), (3, 0), (0, 3), (0, 0))
LANES = 128
WIDE = NQ * LANES
KP = NQ * BP + 8
PITCH = 264
ORDER = FAR[-1:] + FAR[:-1]


def iota(shape, dim):
    return lax.broadcasted_iota(I32, shape, dim)


def ones_where(mask):
    return jnp.where(mask, 1.0, 0.0).astype(BF16)


def mm(a, b):
    return jnp.dot(a, b, preferred_element_type=F32)


def mm_t(a, b):
    return lax.dot_general(a, b, (((1,), (1,)), ((), ())), preferred_element_type=F32)


def halves(x):
    return jnp.concatenate([x[:, :LANES], x[:, LANES:]], axis=0)


def steps(x, size, count):
    result = jnp.zeros_like(x)
    for k in range(1, count):
        result = result + jnp.where(x >= size * k, 1, 0)
    return result


def face_rows(source, raw):
    raw[...] = jnp.zeros(raw.shape, F32)
    for q in range(FQ):
        for t in range(2):
            raw[8 * q + 4 * t : 8 * q + 4 * t + 4, 0:NB] = source[q]
    return raw[...].astype(BF16)


def kernel(
    state, geometry, material, neighbours, send_faces, vol_eval, vol_grad, face_eval, face_lift,
    normals, areas, out,
    st_v, mat_v, nb_v, sf_v, ve_v, vg_v, fe_v, fl_v, nrm_v, ar_v,
    recv, sendb, xr, sp, sb, raw, ohs, ohr, tr, pts, own, gath, flx, fx, vgm,
    load_sem, gsend_sem, grecv_sem, tsend_sem, trecv_sem, ready_sem,
):
    row, col = lax.axis_index("row"), lax.axis_index("col")
    chip, core = row // 2, row % 2
    cx, cy = chip // 4, chip % 4

    def neighbour(dx, dy):
        return ((cx + dx) & 3) * 4 + ((cy + dy) & 3)

    barrier = pltpu.get_barrier_semaphore()

    def signal(sem, r, c):
        pl.semaphore_signal(sem, inc=1, device_id={"row": r, "col": c}, device_id_type=MESH)

    for d in (4, 3, 5, 2, 6, 1, 7):
        signal(barrier, 2 * chip, lax.rem(col + d, COLS))

    for dx, dy in FAR[:-1]:
        signal(barrier, 2 * neighbour(dx, dy) + 1, col)

    signal(barrier, 2 * chip + (1 - core), col)

    pairs = [
        (state, st_v), (material, mat_v), (neighbours, nb_v), (send_faces, sf_v), (vol_eval, ve_v),
        (vol_grad, vg_v), (face_eval, fe_v), (face_lift, fl_v), (normals, nrm_v), (areas, ar_v),
    ]
    loads = [pltpu.make_async_copy(a, b, load_sem.at[i]) for i, (a, b) in enumerate(pairs)]
    for copy in loads:
        copy.start()

    def block(p):
        return geometry.at[:, pl.ds(2 * p, 2)]

    local = pltpu.make_async_copy(block(row), recv.at[row], grecv_sem.at[row])
    local.start()

    def metric_copy(to, source):
        return pltpu.make_async_remote_copy(
            src_ref=block(to), dst_ref=recv.at[source], send_sem=gsend_sem,
            recv_sem=grecv_sem.at[source], device_id={"row": to, "col": col}, device_id_type=MESH,
        )

    def trace_copy(to, source):
        return pltpu.make_async_remote_copy(
            src_ref=sendb.at[to], dst_ref=xr.at[source], send_sem=tsend_sem,
            recv_sem=trecv_sem, device_id={"row": row, "col": to}, device_id_type=MESH,
        )

    for i in (0, 1, 3, 6):
        loads[i].wait()
    for m in range(NQ):
        sp[m * BP : m * BP + NB, :] = st_v[m]
        sp[m * BP + NB : (m + 1) * BP, :] = jnp.zeros((BP - NB, E), F32)
    high = mat_v[0:3, :].astype(BF16).astype(F32)
    sp[NQ * BP : NQ * BP + 3, :] = high
    sp[NQ * BP + 3 : NQ * BP + 6, :] = mat_v[0:3, :] - high
    sp[NQ * BP + 6 : KP, :] = jnp.zeros((2, E), F32)
    dof = sp[...].astype(BF16)

    eval_rows = face_rows(fe_v, raw.at[0])

    col_kp = iota((1, KP), 1)
    m_col = steps(col_kp, BP, NQ)
    spread9 = ones_where((iota((BP, 1), 0) == col_kp - BP * m_col) & (col_kp < NQ * BP))
    wide_eval = mm(eval_rows, spread9).astype(BF16)
    row_t = iota((256, 1), 0)
    m_row = steps(row_t, FQ, NQ)
    q_row = row_t - FQ * m_row
    same = (m_row == m_col) & (row_t < NQ * FQ) & (col_kp < NQ * BP)
    carry = (row_t - NQ * FQ == col_kp - NQ * BP) & (col_kp >= NQ * BP)
    for f in range(FACES):
        pick = ones_where(iota((1, 8 * FQ), 1) == 8 * q_row + f)
        weights = jnp.where(same, mm(pick, wide_eval), jnp.where(carry, 1.0, 0.0)).astype(BF16)
        tr[:, f * E : (f + 1) * E] = mm(weights, dof).astype(BF16)

    listed = jnp.transpose(jnp.concatenate([sf_v[0], sf_v[0]], axis=1))
    for p in range(COLS):
        ohs[p * SLOTS : (p + 1) * SLOTS, :] = ones_where(
            listed[0:SLOTS, p : p + 1] == iota((1, FACES * E), 1)
        )
    outgoing = mm_t(ohs[...], tr[...]).astype(BF16)
    for p in range(COLS):
        sendb[p] = outgoing[p * SLOTS : (p + 1) * SLOTS, :]
    xr[col] = jnp.zeros((SLOTS, 256), BF16)

    def wait_column():
        @pl.when(core == 0)
        def _():
            pl.semaphore_wait(barrier, 2 * (COLS - 1) + 1)
            signal(ready_sem, row + 1, col)

        @pl.when(core == 1)
        def _():
            pl.semaphore_wait(ready_sem, 1)

    def wait_plane():
        @pl.when(core == 1)
        def _():
            pl.semaphore_wait(barrier, ROWS - 1)
            signal(ready_sem, row - 1, col)

        @pl.when(core == 0)
        def _():
            pl.semaphore_wait(ready_sem, 1)

    def send_traces():
        @pl.loop(0, COLS - 1)
        def _(i):
            trace_copy(i + jnp.where(i >= col, 1, 0), col).start()

    def send_metric():
        for dx, dy in FAR:
            peer = neighbour(dx, dy)
            if (dx, dy) != (0, 0):
                metric_copy(2 * peer + core, row).start()
            metric_copy(2 * peer + (1 - core), row).start()

    @pl.when(col >= EARLY)
    def _():
        wait_column()
        send_traces()
        wait_plane()
        send_metric()

    @pl.when(col < EARLY)
    def _():
        wait_plane()
        send_metric()
        wait_column()
        send_traces()

    for i in (2, 4, 5, 7, 8, 9):
        loads[i].wait()

    for m in range(NQ):
        both = jnp.concatenate(
            [sp[m * BP : (m + 1) * BP, :LANES], sp[m * BP : (m + 1) * BP, LANES:]], axis=0
        )
        sb[:, m * LANES : (m + 1) * LANES] = both.astype(BF16)
    tile_col = jnp.where(iota((1, 2 * BP), 1) >= BP, 1, 0)
    twice = ones_where(iota((BP, 1), 0) == iota((1, 2 * BP), 1) - BP * tile_col)
    face_row = iota((8 * FQ, 1), 0)
    eval_mask = ((face_row >> 2) & 1) == tile_col
    face_weights = jnp.where(eval_mask, mm(eval_rows, twice), 0.0).astype(BF16)
    own[...] = mm(face_weights, sb[...]).reshape(FQ, 8, WIDE)
    point_row = iota((256, 1), 0)
    spread_v = ones_where(iota((1, 128), 1) == 4 * (point_row >> 3) + (point_row & 3))
    pad = jnp.zeros((BP - NB, 128), F32)
    eval2 = jnp.concatenate([ve_v[...], pad, ve_v[...], pad], axis=0).astype(BF16)
    vol_mask = ((point_row >> 2) & 1) == tile_col
    vol_weights = jnp.where(vol_mask, mm_t(spread_v, eval2), 0.0).astype(BF16)
    pts[...] = mm(vol_weights, sb[...])
    tile_row = jnp.where(iota((2 * BP, 1), 0) >= BP, 1, 0)
    grad_mask = tile_row == ((iota((1, 256), 1) >> 2) & 1)
    for d in range(3):
        grad = vg_v[d].astype(F32)
        grad2 = jnp.concatenate([grad, pad, grad, pad], axis=0).astype(BF16)
        vgm[:, d * 256 : (d + 1) * 256] = jnp.where(grad_mask, mm_t(grad2, spread_v), 0.0).astype(BF16)
    twice_t = ones_where(iota((2 * BP, 1), 0) - BP * tile_row == iota((1, BP), 1))
    lift_mask = tile_row == ((iota((1, 8 * FQ), 1) >> 2) & 1)
    lift_rows = face_rows(fl_v, raw.at[1])
    lift = jnp.where(lift_mask, mm_t(twice_t, lift_rows), 0.0).astype(BF16)

    kind, peer, target, turn = nb_v[0], nb_v[1], nb_v[2], nb_v[3]
    face_id = iota((FACES, E), 0) * E + iota((FACES, E), 1)
    code = jnp.where(
        kind == 0, target, jnp.where(kind == 1, FACES * E + peer * SLOTS + target, face_id)
    )
    for f in range(FACES):
        got = mm(tr[...], ones_where(iota((FACES * E, 1), 0) == code[f : f + 1, :]))
        for t in range(2):
            gath[(4 * t + f) * PITCH : (4 * t + f) * PITCH + 256, :] = got[:, t * LANES : (t + 1) * LANES]

        ohr[:, f * E : (f + 1) * E] = ones_where(
            iota((COLS * SLOTS, 1), 0) + FACES * E == code[f : f + 1, :]
        )
    ident = ones_where(iota((256, 1), 0) == iota((1, 256), 1))
    def all_metric():
        part = recv.at[pl.ds(0, ROWS - 1)]
        return pltpu.make_async_remote_copy(
            src_ref=part, dst_ref=part, send_sem=gsend_sem, recv_sem=grecv_sem.at[0],
            device_id={"row": lax.rem(row + 1, ROWS), "col": col}, device_id_type=MESH,
        )

    def chip_products(dx, dy):
        src = neighbour(-dx, -dy)
        for a in range(2):
            metric_copy(2 * src + a, 2 * src + a).wait_recv()
        at = pl.multiple_of(16 * src, 16)
        u = [pts[pl.ds(at, 16), m * LANES : (m + 1) * LANES] for m in range(NQ)]
        for d in range(3):
            n = [
                jnp.concatenate(
                    [got8(recv, 2 * src, 3 * d + j), got8(recv, 2 * src + 1, 3 * d + j)], axis=0
                )
                for j in range(3)
            ]
            product = [
                n[0] * u[6],
                n[1] * u[7],
                n[2] * u[8],
                n[0] * u[7] + n[1] * u[6],
                n[1] * u[8] + n[2] * u[7],
                n[0] * u[8] + n[2] * u[6],
                u[0] * n[0] + u[3] * n[1] + u[5] * n[2],
                u[3] * n[0] + u[1] * n[1] + u[4] * n[2],
                u[5] * n[0] + u[4] * n[1] + u[2] * n[2],
            ]
            for m in range(NQ):
                fx[pl.ds(pl.multiple_of(d * 256 + at, 16), 16), m * LANES : (m + 1) * LANES] = product[
                    m
                ].astype(BF16)

    for dx, dy in ORDER[:12]:
        chip_products(dx, dy)

    def all_traces():
        part = xr.at[pl.ds(0, COLS - 1)]
        return pltpu.make_async_remote_copy(
            src_ref=part, dst_ref=part, send_sem=tsend_sem, recv_sem=trecv_sem,
            device_id={"row": row, "col": lax.rem(col + 1, COLS)}, device_id_type=MESH,
        )

    all_traces().wait_recv()

    xt = mm_t(ident, xr[...].reshape(COLS * SLOTS, 256)).astype(BF16)
    for f in range(FACES):
        got = mm(xt, ohr[:, f * E : (f + 1) * E])
        for t in range(2):
            at = (4 * t + f) * PITCH
            gath[at : at + 256, :] = gath[at : at + 256, :] + got[:, t * LANES : (t + 1) * LANES]

    def gathered(r):
        return gath[pl.ds(r, 8, stride=PITCH), :]

    def per_face(i):
        return jnp.concatenate(
            [jnp.broadcast_to(mat_v[i : i + 1, t * LANES : (t + 1) * LANES], (4, LANES)) for t in range(2)],
            axis=0,
        )

    kind8, turn8 = halves(kind), halves(turn)
    l1, g1, w1 = per_face(0), per_face(1), per_face(2)
    l2, g2, w2 = [gathered(NQ * FQ + i) + gathered(NQ * FQ + 3 + i) for i in range(3)]
    fastest = 0.5 * jnp.maximum(jnp.sqrt((l1 + 2.0 * g1) * w1), jnp.sqrt((l2 + 2.0 * g2) * w2))
    sign_v = jnp.where(kind8 == 3, 0.0, 1.0)
    sign_s = jnp.where(kind8 == 2, -1.0, sign_v)
    l1, g1, w1 = 0.5 * l1, 0.5 * g1, 0.5 * w1
    l2, g2, w2 = 0.5 * l2 * sign_v, 0.5 * g2 * sign_v, 0.5 * w2 * sign_s
    turn_one, turn_two = turn8 == 1, turn8 == 2

    @pl.loop(0, FQ // 3)
    def _(i):
        q0 = 3 * i
        outer = [[], [], []]
        for m in range(NQ):
            g = [gathered(m * FQ + q0 + k) for k in range(3)]
            for k in range(3):
                outer[k].append(
                    jnp.where(turn_one, g[(k + 1) % 3], jnp.where(turn_two, g[(k + 2) % 3], g[k]))
                )
        for k in range(3):
            q = q0 + k
            o = outer[k]
            u = [own[q, :, m * LANES : (m + 1) * LANES] for m in range(NQ)]
            n = [halves(nrm_v[j, q].astype(F32)) for j in range(3)]
            penalty = fastest * halves(ar_v[q])
            rigid = [g1 * u[6 + j] + g2 * o[6 + j] for j in range(3)]
            lame = [l1 * u[6 + j] + l2 * o[6 + j] for j in range(3)]
            stress = [w1 * u[s] + w2 * o[s] for s in range(6)]
            pressure = n[0] * lame[0] + n[1] * lame[1] + n[2] * lame[2]
            flux = [
                pressure + 2.0 * (n[0] * rigid[0]),
                pressure + 2.0 * (n[1] * rigid[1]),
                pressure + 2.0 * (n[2] * rigid[2]),
                n[0] * rigid[1] + n[1] * rigid[0],
                n[1] * rigid[2] + n[2] * rigid[1],
                n[0] * rigid[2] + n[2] * rigid[0],
                stress[0] * n[0] + stress[3] * n[1] + stress[5] * n[2],
                stress[3] * n[0] + stress[1] * n[1] + stress[4] * n[2],
                stress[5] * n[0] + stress[4] * n[1] + stress[2] * n[2],
            ]
            for m in range(NQ):
                sign = sign_s if m < 6 else sign_v
                flx[q, :, m * LANES : (m + 1) * LANES] = penalty * (u[m] - sign * o[m]) - flux[m]

    surface = mm(lift, flx[...].reshape(8 * FQ, WIDE).astype(BF16))

    for dx, dy in ORDER[12:]:
        chip_products(dx, dy)

    all_metric().wait_send()
    all_traces().wait_send()
    volume = mm(vgm[...], fx[...])
    for t in range(2):
        rows = slice(t * BP, (t + 1) * BP)
        lanes = slice(t * LANES, (t + 1) * LANES)
        v = [volume[rows, m * LANES : (m + 1) * LANES] for m in range(NQ)]
        l, g, w, step = [mat_v[i : i + 1, lanes] for i in range(4)]
        pressure = l * (v[0] + v[1] + v[2])
        for m in range(NQ):
            if m < 3:
                total = -(pressure + 2.0 * g * v[m])
            elif m < 6:
                total = -g * v[m]
            else:
                total = -w * v[m]
            total = total - surface[rows, m * LANES : (m + 1) * LANES]
            out[m, :, lanes] = st_v[m, :, lanes] + (step * total)[0:NB]


def got8(recv, r, k):
    return recv[r, k].astype(F32).reshape(8, LANES)


def per_device(
    state, geometry, material, neighbours, send_faces, vol_eval, vol_grad, face_eval, face_lift,
    normals, areas,
):
    geometry = jnp.transpose(geometry.reshape(9, 4, 2 * ROWS, LANES), (0, 2, 1, 3))
    face_eval = jnp.transpose(face_eval, (2, 0, 1))
    face_lift = jnp.transpose(face_lift, (2, 0, 1))
    args = (
        state, geometry, material, neighbours, send_faces, vol_eval, vol_grad, face_eval, face_lift,
        normals, areas,
    )
    args = tuple(pltpu.with_memory_space_constraint(a, pltpu.HBM) for a in args)
    staged = [a for i, a in enumerate(args) if i != 1]
    dma = pltpu.SemaphoreType.DMA
    return pl.pallas_call(
        kernel,
        out_shape=jax.ShapeDtypeStruct((NQ, NB, E), F32),
        in_specs=[pl.BlockSpec(memory_space=pl.ANY)] * len(args),
        out_specs=pl.BlockSpec(memory_space=pltpu.VMEM),
        scratch_shapes=[pltpu.VMEM(a.shape, a.dtype) for a in staged]
        + [
            pltpu.VMEM((ROWS, 9, 2, 4, LANES), BF16),
            pltpu.VMEM((COLS, SLOTS, 256), BF16),
            pltpu.VMEM((COLS, SLOTS, 256), BF16),
            pltpu.VMEM((KP, E), F32),
            pltpu.VMEM((2 * BP, WIDE), BF16),
            pltpu.VMEM((2, 8 * FQ, BP), F32),
            pltpu.VMEM((COLS * SLOTS, FACES * E), BF16),
            pltpu.VMEM((COLS * SLOTS, FACES * E), BF16),
            pltpu.VMEM((256, FACES * E), BF16),
            pltpu.VMEM((256, WIDE), F32),
            pltpu.VMEM((FQ, 8, WIDE), F32),
            pltpu.VMEM((8 * PITCH, LANES), F32),
            pltpu.VMEM((FQ, 8, WIDE), F32),
            pltpu.VMEM((3 * 256, WIDE), BF16),
            pltpu.VMEM((2 * BP, 3 * 256), BF16),
            dma((len(staged),)), pltpu.SemaphoreType.DMA, dma((ROWS,)), pltpu.SemaphoreType.DMA, pltpu.SemaphoreType.DMA,
            pltpu.SemaphoreType.REGULAR,
        ],
        compiler_params=pltpu.CompilerParams(
            collective_id=0, has_side_effects=True, vmem_limit_bytes=40 * 1024 * 1024
        ),
        name="section",
    )(*args)


def solution(mesh):
    blocks = P(None, None, ("col", "row"))
    in_specs = (
        blocks, P(None, "row", "col"), P(None, ("col", "row")), blocks, P(("col", "row"), None, None),
        P(), P(), P(), P(), P(None, None, None, ("col", "row")), blocks,
    )
    return jax.shard_map(
        per_device, mesh=mesh, in_specs=in_specs, out_specs=blocks, check_vma=False
    )
```

```python
import jax
import jax.numpy as jnp
from jax import lax
from jax.experimental import pallas as pl
from jax.experimental.pallas import tpu as pltpu
from jax.sharding import PartitionSpec as P

MESH = pl.DeviceIdType.MESH
F32, BF16, I32 = jnp.float32, jnp.bfloat16, jnp.int32

NQ, NB, BP = 9, 35, 40
FQ, FACES, E = 27, 4, 256
ROWS, COLS, SLOTS = 32, 8, 64
CHIPS = ROWS // 2
EARLY = 4
FAR = ((2, 2), (2, 1), (1, 2), (2, 3), (3, 2), (2, 0), (0, 2), (1, 1), (3, 3), (1, 3), (3, 1), (1, 0), (0, 1), (3, 0), (0, 3), (0, 0))
LANES = 128
WIDE = NQ * LANES
KP = NQ * BP + 8
PITCH = 264
ORDER = FAR[-1:] + FAR[:-1]


def iota(shape, dim):
    return lax.broadcasted_iota(I32, shape, dim)


def ones_where(mask):
    return jnp.where(mask, 1.0, 0.0).astype(BF16)


def mm(a, b):
    return jnp.dot(a, b, preferred_element_type=F32)


def mm_t(a, b):
    return lax.dot_general(a, b, (((1,), (1,)), ((), ())), preferred_element_type=F32)


def halves(x):
    return jnp.concatenate([x[:, :LANES], x[:, LANES:]], axis=0)


def steps(x, size, count):
    result = jnp.zeros_like(x)
    for k in range(1, count):
        result = result + jnp.where(x >= size * k, 1, 0)
    return result


def face_rows(source, raw):
    raw[...] = jnp.zeros(raw.shape, F32)
    for q in range(FQ):
        for t in range(2):
            raw[8 * q + 4 * t : 8 * q + 4 * t + 4, 0:NB] = source[q]
    return raw[...].astype(BF16)


def kernel(
    state, geometry, material, neighbours, send_faces, vol_eval, vol_grad, face_eval, face_lift,
    normals, areas, out,
    geo_v, st_v, mat_v, nb_v, sf_v, ve_v, vg_v, fe_v, fl_v, nrm_v, ar_v,
    recv, sendb, xr, sp, sb, raw, ohs, ohr, tr, pts, own, gath, flx, fx, vgm,
    load_sem, gsend_sem, grecv_sem, tsend_sem, trecv_sem, ready_sem,
):
    row, col = lax.axis_index("row"), lax.axis_index("col")
    chip, core = row // 2, row % 2
    cx, cy = chip // 4, chip % 4

    def neighbour(dx, dy):
        return ((cx + dx) & 3) * 4 + ((cy + dy) & 3)

    barrier = pltpu.get_barrier_semaphore()

    def signal(sem, r, c):
        pl.semaphore_signal(sem, inc=1, device_id={"row": r, "col": c}, device_id_type=MESH)

    for d in (4, 3, 5, 2, 6, 1, 7):
        signal(barrier, 2 * chip, lax.rem(col + d, COLS))

    for dx, dy in FAR[:-1]:
        signal(barrier, 2 * neighbour(dx, dy) + 1, col)

    signal(barrier, 2 * chip + (1 - core), col)

    pairs = [
        (state, st_v), (material, mat_v), (neighbours, nb_v), (send_faces, sf_v), (vol_eval, ve_v),
        (vol_grad, vg_v), (face_eval, fe_v), (face_lift, fl_v), (normals, nrm_v), (areas, ar_v),
    ]
    loads = [pltpu.make_async_copy(a, b, load_sem.at[i]) for i, (a, b) in enumerate(pairs)]
    for copy in loads:
        copy.start()

    stage = pltpu.make_async_copy(geometry, geo_v, load_sem.at[len(pairs)])
    stage.start()
    local = pltpu.make_async_copy(
        geometry.at[:, pl.ds(2 * row, 2)], recv.at[row], grecv_sem.at[row]
    )
    local.start()

    def block(p):
        return geo_v.at[:, pl.ds(2 * p, 2)]


    def metric_copy(to, source):
        return pltpu.make_async_remote_copy(
            src_ref=block(to), dst_ref=recv.at[source], send_sem=gsend_sem,
            recv_sem=grecv_sem.at[source], device_id={"row": to, "col": col}, device_id_type=MESH,
        )

    def trace_copy(to, source):
        return pltpu.make_async_remote_copy(
            src_ref=sendb.at[to], dst_ref=xr.at[source], send_sem=tsend_sem,
            recv_sem=trecv_sem, device_id={"row": row, "col": to}, device_id_type=MESH,
        )

    for i in (0, 1, 3, 6):
        loads[i].wait()
    for m in range(NQ):
        sp[m * BP : m * BP + NB, :] = st_v[m]
        sp[m * BP + NB : (m + 1) * BP, :] = jnp.zeros((BP - NB, E), F32)
    high = mat_v[0:3, :].astype(BF16).astype(F32)
    sp[NQ * BP : NQ * BP + 3, :] = high
    sp[NQ * BP + 3 : NQ * BP + 6, :] = mat_v[0:3, :] - high
    sp[NQ * BP + 6 : KP, :] = jnp.zeros((2, E), F32)
    dof = sp[...].astype(BF16)

    eval_rows = face_rows(fe_v, raw.at[0])

    col_kp = iota((1, KP), 1)
    m_col = steps(col_kp, BP, NQ)
    spread9 = ones_where((iota((BP, 1), 0) == col_kp - BP * m_col) & (col_kp < NQ * BP))
    wide_eval = mm(eval_rows, spread9).astype(BF16)
    row_t = iota((256, 1), 0)
    m_row = steps(row_t, FQ, NQ)
    q_row = row_t - FQ * m_row
    same = (m_row == m_col) & (row_t < NQ * FQ) & (col_kp < NQ * BP)
    carry = (row_t - NQ * FQ == col_kp - NQ * BP) & (col_kp >= NQ * BP)
    for f in range(FACES):
        pick = ones_where(iota((1, 8 * FQ), 1) == 8 * q_row + f)
        weights = jnp.where(same, mm(pick, wide_eval), jnp.where(carry, 1.0, 0.0)).astype(BF16)
        tr[:, f * E : (f + 1) * E] = mm(weights, dof).astype(BF16)

    listed = jnp.transpose(jnp.concatenate([sf_v[0], sf_v[0]], axis=1))
    for p in range(COLS):
        ohs[p * SLOTS : (p + 1) * SLOTS, :] = ones_where(
            listed[0:SLOTS, p : p + 1] == iota((1, FACES * E), 1)
        )
    outgoing = mm_t(ohs[...], tr[...]).astype(BF16)
    for p in range(COLS):
        sendb[p] = outgoing[p * SLOTS : (p + 1) * SLOTS, :]
    xr[col] = jnp.zeros((SLOTS, 256), BF16)

    def wait_column():
        @pl.when(core == 0)
        def _():
            pl.semaphore_wait(barrier, 2 * (COLS - 1) + 1)
            signal(ready_sem, row + 1, col)

        @pl.when(core == 1)
        def _():
            pl.semaphore_wait(ready_sem, 1)

    def wait_plane():
        @pl.when(core == 1)
        def _():
            pl.semaphore_wait(barrier, ROWS - 1)
            signal(ready_sem, row - 1, col)

        @pl.when(core == 0)
        def _():
            pl.semaphore_wait(ready_sem, 1)

    def send_traces():
        @pl.loop(0, COLS - 1)
        def _(i):
            trace_copy(i + jnp.where(i >= col, 1, 0), col).start()

    def send_metric():
        stage.wait()
        for dx, dy in FAR:
            peer = neighbour(dx, dy)
            if (dx, dy) != (0, 0):
                metric_copy(2 * peer + core, row).start()
            metric_copy(2 * peer + (1 - core), row).start()

    @pl.when(col >= EARLY)
    def _():
        wait_column()
        send_traces()
        wait_plane()
        send_metric()

    @pl.when(col < EARLY)
    def _():
        wait_plane()
        send_metric()
        wait_column()
        send_traces()

    for i in (2, 4, 5, 7, 8, 9):
        loads[i].wait()

    for m in range(NQ):
        both = jnp.concatenate(
            [sp[m * BP : (m + 1) * BP, :LANES], sp[m * BP : (m + 1) * BP, LANES:]], axis=0
        )
        sb[:, m * LANES : (m + 1) * LANES] = both.astype(BF16)
    tile_col = jnp.where(iota((1, 2 * BP), 1) >= BP, 1, 0)
    twice = ones_where(iota((BP, 1), 0) == iota((1, 2 * BP), 1) - BP * tile_col)
    face_row = iota((8 * FQ, 1), 0)
    eval_mask = ((face_row >> 2) & 1) == tile_col
    face_weights = jnp.where(eval_mask, mm(eval_rows, twice), 0.0).astype(BF16)
    own[...] = mm(face_weights, sb[...]).reshape(FQ, 8, WIDE)
    point_row = iota((256, 1), 0)
    spread_v = ones_where(iota((1, 128), 1) == 4 * (point_row >> 3) + (point_row & 3))
    pad = jnp.zeros((BP - NB, 128), F32)
    eval2 = jnp.concatenate([ve_v[...], pad, ve_v[...], pad], axis=0).astype(BF16)
    vol_mask = ((point_row >> 2) & 1) == tile_col
    vol_weights = jnp.where(vol_mask, mm_t(spread_v, eval2), 0.0).astype(BF16)
    pts[...] = mm(vol_weights, sb[...])
    tile_row = jnp.where(iota((2 * BP, 1), 0) >= BP, 1, 0)
    grad_mask = tile_row == ((iota((1, 256), 1) >> 2) & 1)
    for d in range(3):
        grad = vg_v[d].astype(F32)
        grad2 = jnp.concatenate([grad, pad, grad, pad], axis=0).astype(BF16)
        vgm[:, d * 256 : (d + 1) * 256] = jnp.where(grad_mask, mm_t(grad2, spread_v), 0.0).astype(BF16)
    twice_t = ones_where(iota((2 * BP, 1), 0) - BP * tile_row == iota((1, BP), 1))
    lift_mask = tile_row == ((iota((1, 8 * FQ), 1) >> 2) & 1)
    lift_rows = face_rows(fl_v, raw.at[1])
    lift = jnp.where(lift_mask, mm_t(twice_t, lift_rows), 0.0).astype(BF16)

    kind, peer, target, turn = nb_v[0], nb_v[1], nb_v[2], nb_v[3]
    face_id = iota((FACES, E), 0) * E + iota((FACES, E), 1)
    code = jnp.where(
        kind == 0, target, jnp.where(kind == 1, FACES * E + peer * SLOTS + target, face_id)
    )
    for f in range(FACES):
        got = mm(tr[...], ones_where(iota((FACES * E, 1), 0) == code[f : f + 1, :]))
        for t in range(2):
            gath[(4 * t + f) * PITCH : (4 * t + f) * PITCH + 256, :] = got[:, t * LANES : (t + 1) * LANES]

        ohr[:, f * E : (f + 1) * E] = ones_where(
            iota((COLS * SLOTS, 1), 0) + FACES * E == code[f : f + 1, :]
        )
    ident = ones_where(iota((256, 1), 0) == iota((1, 256), 1))
    def all_metric():
        part = recv.at[pl.ds(0, ROWS - 1)]
        return pltpu.make_async_remote_copy(
            src_ref=part, dst_ref=part, send_sem=gsend_sem, recv_sem=grecv_sem.at[0],
            device_id={"row": lax.rem(row + 1, ROWS), "col": col}, device_id_type=MESH,
        )

    def chip_products(dx, dy):
        src = neighbour(-dx, -dy)
        for a in range(2):
            metric_copy(2 * src + a, 2 * src + a).wait_recv()
        at = pl.multiple_of(16 * src, 16)
        u = [pts[pl.ds(at, 16), m * LANES : (m + 1) * LANES] for m in range(NQ)]
        for d in range(3):
            n = [
                jnp.concatenate(
                    [got8(recv, 2 * src, 3 * d + j), got8(recv, 2 * src + 1, 3 * d + j)], axis=0
                )
                for j in range(3)
            ]
            product = [
                n[0] * u[6],
                n[1] * u[7],
                n[2] * u[8],
                n[0] * u[7] + n[1] * u[6],
                n[1] * u[8] + n[2] * u[7],
                n[0] * u[8] + n[2] * u[6],
                u[0] * n[0] + u[3] * n[1] + u[5] * n[2],
                u[3] * n[0] + u[1] * n[1] + u[4] * n[2],
                u[5] * n[0] + u[4] * n[1] + u[2] * n[2],
            ]
            for m in range(NQ):
                fx[pl.ds(pl.multiple_of(d * 256 + at, 16), 16), m * LANES : (m + 1) * LANES] = product[
                    m
                ].astype(BF16)

    for dx, dy in ORDER[:12]:
        chip_products(dx, dy)

    def all_traces():
        part = xr.at[pl.ds(0, COLS - 1)]
        return pltpu.make_async_remote_copy(
            src_ref=part, dst_ref=part, send_sem=tsend_sem, recv_sem=trecv_sem,
            device_id={"row": row, "col": lax.rem(col + 1, COLS)}, device_id_type=MESH,
        )

    all_traces().wait_recv()

    xt = mm_t(ident, xr[...].reshape(COLS * SLOTS, 256)).astype(BF16)
    for f in range(FACES):
        got = mm(xt, ohr[:, f * E : (f + 1) * E])
        for t in range(2):
            at = (4 * t + f) * PITCH
            gath[at : at + 256, :] = gath[at : at + 256, :] + got[:, t * LANES : (t + 1) * LANES]

    def gathered(r):
        return gath[pl.ds(r, 8, stride=PITCH), :]

    def per_face(i):
        return jnp.concatenate(
            [jnp.broadcast_to(mat_v[i : i + 1, t * LANES : (t + 1) * LANES], (4, LANES)) for t in range(2)],
            axis=0,
        )

    kind8, turn8 = halves(kind), halves(turn)
    l1, g1, w1 = per_face(0), per_face(1), per_face(2)
    l2, g2, w2 = [gathered(NQ * FQ + i) + gathered(NQ * FQ + 3 + i) for i in range(3)]
    fastest = 0.5 * jnp.maximum(jnp.sqrt((l1 + 2.0 * g1) * w1), jnp.sqrt((l2 + 2.0 * g2) * w2))
    sign_v = jnp.where(kind8 == 3, 0.0, 1.0)
    sign_s = jnp.where(kind8 == 2, -1.0, sign_v)
    l1, g1, w1 = 0.5 * l1, 0.5 * g1, 0.5 * w1
    l2, g2, w2 = 0.5 * l2 * sign_v, 0.5 * g2 * sign_v, 0.5 * w2 * sign_s
    turn_one, turn_two = turn8 == 1, turn8 == 2

    @pl.loop(0, FQ // 3)
    def _(i):
        q0 = 3 * i
        outer = [[], [], []]
        for m in range(NQ):
            g = [gathered(m * FQ + q0 + k) for k in range(3)]
            for k in range(3):
                outer[k].append(
                    jnp.where(turn_one, g[(k + 1) % 3], jnp.where(turn_two, g[(k + 2) % 3], g[k]))
                )
        for k in range(3):
            q = q0 + k
            o = outer[k]
            u = [own[q, :, m * LANES : (m + 1) * LANES] for m in range(NQ)]
            n = [halves(nrm_v[j, q].astype(F32)) for j in range(3)]
            penalty = fastest * halves(ar_v[q])
            rigid = [g1 * u[6 + j] + g2 * o[6 + j] for j in range(3)]
            lame = [l1 * u[6 + j] + l2 * o[6 + j] for j in range(3)]
            stress = [w1 * u[s] + w2 * o[s] for s in range(6)]
            pressure = n[0] * lame[0] + n[1] * lame[1] + n[2] * lame[2]
            flux = [
                pressure + 2.0 * (n[0] * rigid[0]),
                pressure + 2.0 * (n[1] * rigid[1]),
                pressure + 2.0 * (n[2] * rigid[2]),
                n[0] * rigid[1] + n[1] * rigid[0],
                n[1] * rigid[2] + n[2] * rigid[1],
                n[0] * rigid[2] + n[2] * rigid[0],
                stress[0] * n[0] + stress[3] * n[1] + stress[5] * n[2],
                stress[3] * n[0] + stress[1] * n[1] + stress[4] * n[2],
                stress[5] * n[0] + stress[4] * n[1] + stress[2] * n[2],
            ]
            for m in range(NQ):
                sign = sign_s if m < 6 else sign_v
                flx[q, :, m * LANES : (m + 1) * LANES] = penalty * (u[m] - sign * o[m]) - flux[m]

    surface = mm(lift, flx[...].reshape(8 * FQ, WIDE).astype(BF16))

    for dx, dy in ORDER[12:]:
        chip_products(dx, dy)

    all_metric().wait_send()
    all_traces().wait_send()
    volume = mm(vgm[...], fx[...])
    for t in range(2):
        rows = slice(t * BP, (t + 1) * BP)
        lanes = slice(t * LANES, (t + 1) * LANES)
        v = [volume[rows, m * LANES : (m + 1) * LANES] for m in range(NQ)]
        l, g, w, step = [mat_v[i : i + 1, lanes] for i in range(4)]
        pressure = l * (v[0] + v[1] + v[2])
        for m in range(NQ):
            if m < 3:
                total = -(pressure + 2.0 * g * v[m])
            elif m < 6:
                total = -g * v[m]
            else:
                total = -w * v[m]
            total = total - surface[rows, m * LANES : (m + 1) * LANES]
            out[m, :, lanes] = st_v[m, :, lanes] + (step * total)[0:NB]


def got8(recv, r, k):
    return recv[r, k].astype(F32).reshape(8, LANES)


def per_device(
    state, geometry, material, neighbours, send_faces, vol_eval, vol_grad, face_eval, face_lift,
    normals, areas,
):
    geometry = jnp.transpose(geometry.reshape(9, 4, 2 * ROWS, LANES), (0, 2, 1, 3))
    face_eval = jnp.transpose(face_eval, (2, 0, 1))
    face_lift = jnp.transpose(face_lift, (2, 0, 1))
    args = (
        state, geometry, material, neighbours, send_faces, vol_eval, vol_grad, face_eval, face_lift,
        normals, areas,
    )
    args = tuple(pltpu.with_memory_space_constraint(a, pltpu.HBM) for a in args)
    staged = [a for i, a in enumerate(args) if i != 1]
    dma = pltpu.SemaphoreType.DMA
    return pl.pallas_call(
        kernel,
        out_shape=jax.ShapeDtypeStruct((NQ, NB, E), F32),
        in_specs=[pl.BlockSpec(memory_space=pl.ANY)] * len(args),
        out_specs=pl.BlockSpec(memory_space=pltpu.VMEM),
        scratch_shapes=[pltpu.VMEM(a.shape, a.dtype) for a in (args[1], *staged)]
        + [
            pltpu.VMEM((ROWS, 9, 2, 4, LANES), BF16),
            pltpu.VMEM((COLS, SLOTS, 256), BF16),
            pltpu.VMEM((COLS, SLOTS, 256), BF16),
            pltpu.VMEM((KP, E), F32),
            pltpu.VMEM((2 * BP, WIDE), BF16),
            pltpu.VMEM((2, 8 * FQ, BP), F32),
            pltpu.VMEM((COLS * SLOTS, FACES * E), BF16),
            pltpu.VMEM((COLS * SLOTS, FACES * E), BF16),
            pltpu.VMEM((256, FACES * E), BF16),
            pltpu.VMEM((256, WIDE), F32),
            pltpu.VMEM((FQ, 8, WIDE), F32),
            pltpu.VMEM((8 * PITCH, LANES), F32),
            pltpu.VMEM((FQ, 8, WIDE), F32),
            pltpu.VMEM((3 * 256, WIDE), BF16),
            pltpu.VMEM((2 * BP, 3 * 256), BF16),
            dma((len(args),)), pltpu.SemaphoreType.DMA, dma((ROWS,)), pltpu.SemaphoreType.DMA, pltpu.SemaphoreType.DMA,
            pltpu.SemaphoreType.REGULAR,
        ],
        compiler_params=pltpu.CompilerParams(
            collective_id=0, has_side_effects=True, vmem_limit_bytes=40 * 1024 * 1024
        ),
        name="section",
    )(*args)


def solution(mesh):
    blocks = P(None, None, ("col", "row"))
    in_specs = (
        blocks, P(None, "row", "col"), P(None, ("col", "row")), blocks, P(("col", "row"), None, None),
        P(), P(), P(), P(), P(None, None, None, ("col", "row")), blocks,
    )
    return jax.shard_map(
        per_device, mesh=mesh, in_specs=in_specs, out_specs=blocks, check_vma=False
    )
```

```python
import jax
import jax.numpy as jnp
from jax import lax
from jax.experimental import pallas as pl
from jax.experimental.pallas import tpu as pltpu
from jax.sharding import PartitionSpec as P

MESH = pl.DeviceIdType.MESH
F32, BF16, I32 = jnp.float32, jnp.bfloat16, jnp.int32

NQ, NB, BP = 9, 35, 40
FQ, FACES, E = 27, 4, 256
ROWS, COLS, SLOTS = 32, 8, 64
CHIPS = ROWS // 2
EARLY = 4
FAR = ((2, 2), (2, 1), (1, 2), (2, 3), (3, 2), (2, 0), (0, 2), (1, 1), (3, 3), (1, 3), (3, 1), (1, 0), (0, 1), (3, 0), (0, 3), (0, 0))
LANES = 128
WIDE = NQ * LANES
KP = NQ * BP + 8
PITCH = 264
ORDER = FAR[-1:] + FAR[:-1]
FIRST, LAST = ORDER[:12], ORDER[12:]


def iota(shape, dim):
    return lax.broadcasted_iota(I32, shape, dim)


def ones_where(mask):
    return jnp.where(mask, 1.0, 0.0).astype(BF16)


def mm(a, b):
    return jnp.dot(a, b, preferred_element_type=F32)


def mm_t(a, b):
    return lax.dot_general(a, b, (((1,), (1,)), ((), ())), preferred_element_type=F32)


def halves(x):
    return jnp.concatenate([x[:, :LANES], x[:, LANES:]], axis=0)


def steps(x, size, count):
    result = jnp.zeros_like(x)
    for k in range(1, count):
        result = result + jnp.where(x >= size * k, 1, 0)
    return result


def face_rows(source, raw):
    raw[...] = jnp.zeros(raw.shape, F32)
    for q in range(FQ):
        for t in range(2):
            raw[8 * q + 4 * t : 8 * q + 4 * t + 4, 0:NB] = source[q]
    return raw[...].astype(BF16)


def face_flux(u, lame, rigid, buoyancy, n):
    r = [rigid * u[6 + j] for j in range(3)]
    s = [buoyancy * u[i] for i in range(6)]
    pressure = lame * (n[0] * u[6] + n[1] * u[7] + n[2] * u[8])
    return [
        pressure + 2.0 * (n[0] * r[0]),
        pressure + 2.0 * (n[1] * r[1]),
        pressure + 2.0 * (n[2] * r[2]),
        n[0] * r[1] + n[1] * r[0],
        n[1] * r[2] + n[2] * r[1],
        n[0] * r[2] + n[2] * r[0],
        s[0] * n[0] + s[3] * n[1] + s[5] * n[2],
        s[3] * n[0] + s[1] * n[1] + s[4] * n[2],
        s[5] * n[0] + s[4] * n[1] + s[2] * n[2],
    ]


def kernel(
    state, geometry, material, neighbours, send_faces, vol_eval, vol_grad, face_eval, face_lift,
    normals, areas, out,
    geo_v, st_v, mat_v, nb_v, sf_v, ve_v, vg_v, fe_v, fl_v, nrm_v, ar_v,
    recv, sendb, xr, sp, sb, raw, ohs, ohr, tr, pts, own, gath, flx, fx_a, fx_b, vg_a, vg_b, acc, base, geo8,
    load_sem, gsend_sem, grecv_sem, tsend_sem, trecv_sem, ready_sem,
):
    row, col = lax.axis_index("row"), lax.axis_index("col")
    chip, core = row // 2, row % 2
    cx, cy = chip // 4, chip % 4

    pairs = [
        (state, st_v), (material, mat_v), (neighbours, nb_v), (send_faces, sf_v), (vol_eval, ve_v),
        (vol_grad, vg_v), (face_eval, fe_v), (face_lift, fl_v), (normals, nrm_v), (areas, ar_v),
    ]
    loads = [pltpu.make_async_copy(a, b, load_sem.at[i]) for i, (a, b) in enumerate(pairs)]
    for i in (0, 6, 3, 1):
        loads[i].start()

    def neighbour(dx, dy):
        return ((cx + dx) & 3) * 4 + ((cy + dy) & 3)

    barrier = pltpu.get_barrier_semaphore()

    def signal(sem, r, c):
        pl.semaphore_signal(sem, inc=1, device_id={"row": r, "col": c}, device_id_type=MESH)

    for d in (4, 3, 5, 2, 6, 1, 7):
        signal(barrier, 2 * chip, lax.rem(col + d, COLS))

    for dx, dy in FAR[:-1]:
        signal(barrier, 2 * neighbour(dx, dy) + 1, col)

    signal(barrier, 2 * chip + (1 - core), col)

    for i in (2, 4, 5, 7, 8, 9):
        loads[i].start()
    stage = pltpu.make_async_copy(geometry, geo_v, load_sem.at[len(pairs)])
    stage.start()
    local = pltpu.make_async_copy(
        geometry.at[:, pl.ds(2 * row, 2)], recv.at[row], grecv_sem.at[row]
    )
    local.start()

    def block(p):
        return geo_v.at[:, pl.ds(2 * p, 2)]


    def metric_copy(to, source):
        return pltpu.make_async_remote_copy(
            src_ref=block(to), dst_ref=recv.at[source], send_sem=gsend_sem,
            recv_sem=grecv_sem.at[source], device_id={"row": to, "col": col}, device_id_type=MESH,
        )

    def trace_copy(to, source):
        return pltpu.make_async_remote_copy(
            src_ref=sendb.at[to], dst_ref=xr.at[source], send_sem=tsend_sem,
            recv_sem=trecv_sem, device_id={"row": row, "col": to}, device_id_type=MESH,
        )

    for i in (0, 1, 3, 6):
        loads[i].wait()
    for m in range(NQ):
        sp[m * BP : m * BP + NB, :] = st_v[m]
        sp[m * BP + NB : (m + 1) * BP, :] = jnp.zeros((BP - NB, E), F32)
    high = mat_v[0:3, :].astype(BF16).astype(F32)
    sp[NQ * BP : NQ * BP + 3, :] = high
    sp[NQ * BP + 3 : NQ * BP + 6, :] = mat_v[0:3, :] - high
    sp[NQ * BP + 6 : KP, :] = jnp.zeros((2, E), F32)
    dof = sp[...].astype(BF16)

    eval_rows = face_rows(fe_v, raw.at[0])

    col_kp = iota((1, KP), 1)
    m_col = steps(col_kp, BP, NQ)
    spread9 = ones_where((iota((BP, 1), 0) == col_kp - BP * m_col) & (col_kp < NQ * BP))
    wide_eval = mm(eval_rows, spread9).astype(BF16)
    row_t = iota((256, 1), 0)
    m_row = steps(row_t, FQ, NQ)
    q_row = row_t - FQ * m_row
    same = (m_row == m_col) & (row_t < NQ * FQ) & (col_kp < NQ * BP)
    carry = (row_t - NQ * FQ == col_kp - NQ * BP) & (col_kp >= NQ * BP)
    for f in range(FACES):
        pick = ones_where(iota((1, 8 * FQ), 1) == 8 * q_row + f)
        weights = jnp.where(same, mm(pick, wide_eval), jnp.where(carry, 1.0, 0.0)).astype(BF16)
        tr[:, f * E : (f + 1) * E] = mm(weights, dof).astype(BF16)

    listed = jnp.transpose(jnp.concatenate([sf_v[0], sf_v[0]], axis=1))
    for p in range(COLS):
        ohs[p * SLOTS : (p + 1) * SLOTS, :] = ones_where(
            listed[0:SLOTS, p : p + 1] == iota((1, FACES * E), 1)
        )
    outgoing = mm_t(ohs[...], tr[...]).astype(BF16)
    for p in range(COLS):
        sendb[p] = outgoing[p * SLOTS : (p + 1) * SLOTS, :]
    xr[col] = jnp.zeros((SLOTS, 256), BF16)

    def wait_column():
        @pl.when(core == 0)
        def _():
            pl.semaphore_wait(barrier, 2 * (COLS - 1) + 1)
            signal(ready_sem, row + 1, col)

        @pl.when(core == 1)
        def _():
            pl.semaphore_wait(ready_sem, 1)

    def wait_plane():
        @pl.when(core == 1)
        def _():
            pl.semaphore_wait(barrier, ROWS - 1)
            signal(ready_sem, row - 1, col)

        @pl.when(core == 0)
        def _():
            pl.semaphore_wait(ready_sem, 1)

    def send_traces():
        @pl.loop(0, COLS - 1)
        def _(i):
            trace_copy(i + jnp.where(i >= col, 1, 0), col).start()

    def send_metric():
        stage.wait()
        far = (chip != 0) & (col == 0)

        @pl.when(far)
        def _():
            metric_copy(1, row).start()

        for dx, dy in FAR[:-1]:
            peer = neighbour(dx, dy)

            @pl.when(jnp.logical_not(far & (peer == 0)))
            def _(peer=peer):
                metric_copy(2 * peer + 1, row).start()

            metric_copy(2 * peer, row).start()
        metric_copy(2 * chip + (1 - core), row).start()

    @pl.when(col >= EARLY)
    def _():
        wait_column()
        send_traces()
        wait_plane()
        send_metric()

    @pl.when(col < EARLY)
    def _():
        wait_plane()
        send_metric()
        wait_column()
        send_traces()

    for i in (2, 4, 5, 7, 8, 9):
        loads[i].wait()

    for m in range(NQ):
        both = jnp.concatenate(
            [sp[m * BP : (m + 1) * BP, :LANES], sp[m * BP : (m + 1) * BP, LANES:]], axis=0
        )
        sb[:, m * LANES : (m + 1) * LANES] = both.astype(BF16)
    tile_col = jnp.where(iota((1, 2 * BP), 1) >= BP, 1, 0)
    twice = ones_where(iota((BP, 1), 0) == iota((1, 2 * BP), 1) - BP * tile_col)
    face_row = iota((8 * FQ, 1), 0)
    eval_mask = ((face_row >> 2) & 1) == tile_col
    face_weights = jnp.where(eval_mask, mm(eval_rows, twice), 0.0).astype(BF16)
    own[...] = mm(face_weights, sb[...]).reshape(FQ, 8, WIDE)
    point_row = iota((256, 1), 0)
    spread_v = ones_where(iota((1, 128), 1) == 4 * (point_row >> 3) + (point_row & 3))
    pad = jnp.zeros((BP - NB, 128), F32)
    eval2 = jnp.concatenate([ve_v[...], pad, ve_v[...], pad], axis=0).astype(BF16)
    vol_mask = ((point_row >> 2) & 1) == tile_col
    vol_weights = jnp.where(vol_mask, mm_t(spread_v, eval2), 0.0).astype(BF16)
    pts[...] = mm(vol_weights, sb[...])
    tile_row = jnp.where(iota((2 * BP, 1), 0) >= BP, 1, 0)
    grads = []
    for d in range(3):
        grad = vg_v[d].astype(F32)
        grads.append(jnp.concatenate([grad, pad, grad, pad], axis=0).astype(BF16))
    for part, weights in ((FIRST, vg_a), (LAST, vg_b)):
        size = 16 * len(part)
        at_row = iota((size, 1), 0)
        source = jnp.zeros((size, 1), I32)
        for i, (dx, dy) in enumerate(part):
            source = jnp.where((at_row >> 4) == i, neighbour(-dx, -dy), source)
        point = 8 * source + 4 * ((at_row >> 3) & 1) + (at_row & 3)
        spread = ones_where(iota((1, 128), 1) == point)
        grad_mask = tile_row == ((iota((1, size), 1) >> 2) & 1)
        for d in range(3):
            weights[:, d * size : (d + 1) * size] = jnp.where(
                grad_mask, mm_t(grads[d], spread), 0.0
            ).astype(BF16)
    twice_t = ones_where(iota((2 * BP, 1), 0) - BP * tile_row == iota((1, BP), 1))
    lift_mask = tile_row == ((iota((1, 8 * FQ), 1) >> 2) & 1)
    lift_rows = face_rows(fl_v, raw.at[1])
    lift = jnp.where(lift_mask, mm_t(twice_t, lift_rows), 0.0).astype(BF16)

    kind, peer, target, turn = nb_v[0], nb_v[1], nb_v[2], nb_v[3]
    face_id = iota((FACES, E), 0) * E + iota((FACES, E), 1)
    code = jnp.where(
        kind == 0, target, jnp.where(kind == 1, FACES * E + peer * SLOTS + target, face_id)
    )
    for f in range(FACES):
        got = mm(tr[...], ones_where(iota((FACES * E, 1), 0) == code[f : f + 1, :]))
        for t in range(2):
            gath[(4 * t + f) * PITCH : (4 * t + f) * PITCH + 256, :] = got[:, t * LANES : (t + 1) * LANES]

        ohr[:, f * E : (f + 1) * E] = ones_where(
            iota((COLS * SLOTS, 1), 0) + FACES * E == code[f : f + 1, :]
        )
    ident = ones_where(iota((256, 1), 0) == iota((1, 256), 1))
    def gathered(r):
        return gath[pl.ds(r, 8, stride=PITCH), :]

    def per_face(i):
        return jnp.concatenate(
            [jnp.broadcast_to(mat_v[i : i + 1, t * LANES : (t + 1) * LANES], (4, LANES)) for t in range(2)],
            axis=0,
        )

    kind8, turn8 = halves(kind), halves(turn)
    l1, g1, w1 = per_face(0), per_face(1), per_face(2)
    speed = jnp.sqrt((l1 + 2.0 * g1) * w1)
    l1, g1, w1 = 0.5 * l1, 0.5 * g1, 0.5 * w1

    @pl.loop(0, FQ)
    def _(q):
        n = [halves(nrm_v[j, q].astype(F32)) for j in range(3)]
        for j in range(3):
            geo8[q, :, j * LANES : (j + 1) * LANES] = n[j]
        geo8[q, :, 3 * LANES : 4 * LANES] = halves(ar_v[q])
        flux = face_flux([own[q, :, m * LANES : (m + 1) * LANES] for m in range(NQ)], l1, g1, w1, n)
        for m in range(NQ):
            base[q, :, m * LANES : (m + 1) * LANES] = -flux[m]

    def all_metric():
        part = recv.at[pl.ds(0, ROWS - 1)]
        return pltpu.make_async_remote_copy(
            src_ref=part, dst_ref=part, send_sem=gsend_sem, recv_sem=grecv_sem.at[0],
            device_id={"row": lax.rem(row + 1, ROWS), "col": col}, device_id_type=MESH,
        )

    def chip_products(dx, dy, i, size, fx):
        src = neighbour(-dx, -dy)
        for a in range(2):
            metric_copy(2 * src + a, 2 * src + a).wait_recv()
        at = pl.multiple_of(16 * src, 16)
        u = [pts[pl.ds(at, 16), m * LANES : (m + 1) * LANES] for m in range(NQ)]
        for d in range(3):
            n = [
                jnp.concatenate(
                    [got8(recv, 2 * src, 3 * d + j), got8(recv, 2 * src + 1, 3 * d + j)], axis=0
                )
                for j in range(3)
            ]
            product = [
                n[0] * u[6],
                n[1] * u[7],
                n[2] * u[8],
                n[0] * u[7] + n[1] * u[6],
                n[1] * u[8] + n[2] * u[7],
                n[0] * u[8] + n[2] * u[6],
                u[0] * n[0] + u[3] * n[1] + u[5] * n[2],
                u[3] * n[0] + u[1] * n[1] + u[4] * n[2],
                u[5] * n[0] + u[4] * n[1] + u[2] * n[2],
            ]
            for m in range(NQ):
                fx[d * size + 16 * i : d * size + 16 * i + 16, m * LANES : (m + 1) * LANES] = product[
                    m
                ].astype(BF16)

    for i, (dx, dy) in enumerate(FIRST):
        chip_products(dx, dy, i, 16 * len(FIRST), fx_a)
    acc[...] = mm(vg_a[...], fx_a[...])

    def all_traces():
        part = xr.at[pl.ds(0, COLS - 1)]
        return pltpu.make_async_remote_copy(
            src_ref=part, dst_ref=part, send_sem=tsend_sem, recv_sem=trecv_sem,
            device_id={"row": row, "col": lax.rem(col + 1, COLS)}, device_id_type=MESH,
        )

    all_traces().wait_recv()

    xt = mm_t(ident, xr[...].reshape(COLS * SLOTS, 256)).astype(BF16)
    for f in range(FACES):
        got = mm(xt, ohr[:, f * E : (f + 1) * E])
        for t in range(2):
            at = (4 * t + f) * PITCH
            gath[at : at + 256, :] = gath[at : at + 256, :] + got[:, t * LANES : (t + 1) * LANES]

    l2, g2, w2 = [gathered(NQ * FQ + i) + gathered(NQ * FQ + 3 + i) for i in range(3)]
    fastest = 0.5 * jnp.maximum(speed, jnp.sqrt((l2 + 2.0 * g2) * w2))
    sign_v = jnp.where(kind8 == 3, 0.0, 1.0)
    sign_s = jnp.where(kind8 == 2, -1.0, sign_v)
    l2, g2, w2 = 0.5 * l2, 0.5 * g2, 0.5 * w2
    turn_one, turn_two = turn8 == 1, turn8 == 2

    @pl.loop(0, FQ // 3)
    def _(i):
        q0 = 3 * i
        outer = [[], [], []]
        for m in range(NQ):
            g = [gathered(m * FQ + q0 + k) for k in range(3)]
            sign = sign_s if m < 6 else sign_v
            for k in range(3):
                outer[k].append(
                    sign
                    * jnp.where(turn_one, g[(k + 1) % 3], jnp.where(turn_two, g[(k + 2) % 3], g[k]))
                )
        for k in range(3):
            q = q0 + k
            n = [geo8[q, :, j * LANES : (j + 1) * LANES] for j in range(3)]
            penalty = fastest * geo8[q, :, 3 * LANES : 4 * LANES]
            flux = face_flux(outer[k], l2, g2, w2, n)
            for m in range(NQ):
                lanes = slice(m * LANES, (m + 1) * LANES)
                flx[q, :, lanes] = penalty * (own[q, :, lanes] - outer[k][m]) + (base[q, :, lanes] - flux[m])

    surface = mm(lift, flx[...].reshape(8 * FQ, WIDE).astype(BF16))

    for i, (dx, dy) in enumerate(LAST):
        chip_products(dx, dy, i, 16 * len(LAST), fx_b)

    all_metric().wait_send()
    all_traces().wait_send()
    volume = acc[...] + mm(vg_b[...], fx_b[...])
    for t in range(2):
        rows = slice(t * BP, (t + 1) * BP)
        lanes = slice(t * LANES, (t + 1) * LANES)
        v = [volume[rows, m * LANES : (m + 1) * LANES] for m in range(NQ)]
        l, g, w, step = [mat_v[i : i + 1, lanes] for i in range(4)]
        pressure = l * (v[0] + v[1] + v[2])
        for m in range(NQ):
            if m < 3:
                total = -(pressure + 2.0 * g * v[m])
            elif m < 6:
                total = -g * v[m]
            else:
                total = -w * v[m]
            total = total - surface[rows, m * LANES : (m + 1) * LANES]
            out[m, :, lanes] = st_v[m, :, lanes] + (step * total)[0:NB]


def got8(recv, r, k):
    return recv[r, k].astype(F32).reshape(8, LANES)


def per_device(
    state, geometry, material, neighbours, send_faces, vol_eval, vol_grad, face_eval, face_lift,
    normals, areas,
):
    geometry = jnp.transpose(geometry.reshape(9, 4, 2 * ROWS, LANES), (0, 2, 1, 3))
    face_eval = jnp.transpose(face_eval, (2, 0, 1))
    face_lift = jnp.transpose(face_lift, (2, 0, 1))
    args = (
        state, geometry, material, neighbours, send_faces, vol_eval, vol_grad, face_eval, face_lift,
        normals, areas,
    )
    args = tuple(pltpu.with_memory_space_constraint(a, pltpu.HBM) for a in args)
    staged = [a for i, a in enumerate(args) if i != 1]
    dma = pltpu.SemaphoreType.DMA
    return pl.pallas_call(
        kernel,
        out_shape=jax.ShapeDtypeStruct((NQ, NB, E), F32),
        in_specs=[pl.BlockSpec(memory_space=pl.ANY)] * len(args),
        out_specs=pl.BlockSpec(memory_space=pltpu.VMEM),
        scratch_shapes=[pltpu.VMEM(a.shape, a.dtype) for a in (args[1], *staged)]
        + [
            pltpu.VMEM((ROWS, 9, 2, 4, LANES), BF16),
            pltpu.VMEM((COLS, SLOTS, 256), BF16),
            pltpu.VMEM((COLS, SLOTS, 256), BF16),
            pltpu.VMEM((KP, E), F32),
            pltpu.VMEM((2 * BP, WIDE), BF16),
            pltpu.VMEM((2, 8 * FQ, BP), F32),
            pltpu.VMEM((COLS * SLOTS, FACES * E), BF16),
            pltpu.VMEM((COLS * SLOTS, FACES * E), BF16),
            pltpu.VMEM((256, FACES * E), BF16),
            pltpu.VMEM((256, WIDE), F32),
            pltpu.VMEM((FQ, 8, WIDE), F32),
            pltpu.VMEM((8 * PITCH, LANES), F32),
            pltpu.VMEM((FQ, 8, WIDE), F32),
            pltpu.VMEM((48 * len(FIRST), WIDE), BF16),
            pltpu.VMEM((48 * len(LAST), WIDE), BF16),
            pltpu.VMEM((2 * BP, 48 * len(FIRST)), BF16),
            pltpu.VMEM((2 * BP, 48 * len(LAST)), BF16),
            pltpu.VMEM((2 * BP, WIDE), F32),
            pltpu.VMEM((FQ, 8, WIDE), F32),
            pltpu.VMEM((FQ, 8, 4 * LANES), F32),
            dma((len(args),)), pltpu.SemaphoreType.DMA, dma((ROWS,)), pltpu.SemaphoreType.DMA, pltpu.SemaphoreType.DMA,
            pltpu.SemaphoreType.REGULAR,
        ],
        compiler_params=pltpu.CompilerParams(
            collective_id=0, has_side_effects=True, vmem_limit_bytes=40 * 1024 * 1024
        ),
        name="section",
    )(*args)


def solution(mesh):
    blocks = P(None, None, ("col", "row"))
    in_specs = (
        blocks, P(None, "row", "col"), P(None, ("col", "row")), blocks, P(("col", "row"), None, None),
        P(), P(), P(), P(), P(None, None, None, ("col", "row")), blocks,
    )
    return jax.shard_map(
        per_device, mesh=mesh, in_specs=in_specs, out_specs=blocks, check_vma=False
    )
```

```python
import jax
import jax.numpy as jnp
from jax import lax
from jax.experimental import pallas as pl
from jax.experimental.pallas import tpu as pltpu
from jax.sharding import PartitionSpec as P

MESH = pl.DeviceIdType.MESH
F32, BF16, I32 = jnp.float32, jnp.bfloat16, jnp.int32

NQ, NB, BP = 9, 35, 40
FQ, FACES, E = 27, 4, 256
ROWS, COLS, SLOTS = 32, 8, 64
CHIPS = ROWS // 2
EARLY = 4
FAR = ((2, 2), (2, 1), (1, 2), (2, 3), (3, 2), (2, 0), (0, 2), (1, 1), (3, 3), (1, 3), (3, 1), (1, 0), (0, 1), (3, 0), (0, 3), (0, 0))
LANES = 128
WIDE = NQ * LANES
KP = NQ * BP + 8
PITCH = 264
ORDER = FAR[-1:] + FAR[:-1]
FIRST, LAST = ORDER[:8], ORDER[8:]


def iota(shape, dim):
    return lax.broadcasted_iota(I32, shape, dim)


def ones_where(mask):
    return jnp.where(mask, 1.0, 0.0).astype(BF16)


def mm(a, b):
    return jnp.dot(a, b, preferred_element_type=F32)


def mm_t(a, b):
    return lax.dot_general(a, b, (((1,), (1,)), ((), ())), preferred_element_type=F32)


def halves(x):
    return jnp.concatenate([x[:, :LANES], x[:, LANES:]], axis=0)


def steps(x, size, count):
    result = jnp.zeros_like(x)
    for k in range(1, count):
        result = result + jnp.where(x >= size * k, 1, 0)
    return result


def face_rows(source, raw):
    raw[...] = jnp.zeros(raw.shape, F32)
    for q in range(FQ):
        for t in range(2):
            raw[8 * q + 4 * t : 8 * q + 4 * t + 4, 0:NB] = source[q]
    return raw[...].astype(BF16)


def face_flux(u, lame, rigid, buoyancy, n):
    r = [rigid * u[6 + j] for j in range(3)]
    s = [buoyancy * u[i] for i in range(6)]
    pressure = lame * (n[0] * u[6] + n[1] * u[7] + n[2] * u[8])
    return [
        pressure + 2.0 * (n[0] * r[0]),
        pressure + 2.0 * (n[1] * r[1]),
        pressure + 2.0 * (n[2] * r[2]),
        n[0] * r[1] + n[1] * r[0],
        n[1] * r[2] + n[2] * r[1],
        n[0] * r[2] + n[2] * r[0],
        s[0] * n[0] + s[3] * n[1] + s[5] * n[2],
        s[3] * n[0] + s[1] * n[1] + s[4] * n[2],
        s[5] * n[0] + s[4] * n[1] + s[2] * n[2],
    ]


def kernel(
    state, geometry, material, neighbours, send_faces, vol_eval, vol_grad, face_eval, face_lift,
    normals, areas, out,
    geo_v, st_v, mat_v, nb_v, sf_v, ve_v, vg_v, fe_v, fl_v, nrm_v, ar_v,
    recv, sendb, xr, sp, sb, raw, ohs, ohr, tr, pts, own, gath, flx, fx_a, fx_b, vg_a, vg_b, acc, base, geo8,
    load_sem, gsend_sem, grecv_sem, tsend_sem, trecv_sem, ready_sem,
):
    row, col = lax.axis_index("row"), lax.axis_index("col")
    chip, core = row // 2, row % 2
    cx, cy = chip // 4, chip % 4

    pairs = [
        (state, st_v), (material, mat_v), (neighbours, nb_v), (send_faces, sf_v), (vol_eval, ve_v),
        (vol_grad, vg_v), (face_eval, fe_v), (face_lift, fl_v), (normals, nrm_v), (areas, ar_v),
    ]
    loads = [pltpu.make_async_copy(a, b, load_sem.at[i]) for i, (a, b) in enumerate(pairs)]
    for i in (0, 6, 3, 1):
        loads[i].start()

    def neighbour(dx, dy):
        return ((cx + dx) & 3) * 4 + ((cy + dy) & 3)

    barrier = pltpu.get_barrier_semaphore()

    def signal(sem, r, c):
        pl.semaphore_signal(sem, inc=1, device_id={"row": r, "col": c}, device_id_type=MESH)

    for dx, dy in FAR[:-1]:
        signal(barrier, 2 * neighbour(dx, dy) + 1, col)

    for d in (4, 3, 5, 2, 6, 1, 7):
        signal(barrier, 2 * chip, lax.rem(col + d, COLS))

    signal(barrier, 2 * chip + (1 - core), col)

    for i in (2, 4, 5, 7, 8, 9):
        loads[i].start()
    stage = pltpu.make_async_copy(geometry, geo_v, load_sem.at[len(pairs)])
    stage.start()
    local = pltpu.make_async_copy(
        geometry.at[:, pl.ds(2 * row, 2)], recv.at[row], grecv_sem.at[row]
    )
    local.start()

    def block(p):
        return geo_v.at[:, pl.ds(2 * p, 2)]


    def metric_copy(to, source):
        return pltpu.make_async_remote_copy(
            src_ref=block(to), dst_ref=recv.at[source], send_sem=gsend_sem,
            recv_sem=grecv_sem.at[source], device_id={"row": to, "col": col}, device_id_type=MESH,
        )

    def trace_copy(to, source):
        return pltpu.make_async_remote_copy(
            src_ref=sendb.at[to], dst_ref=xr.at[source], send_sem=tsend_sem,
            recv_sem=trecv_sem, device_id={"row": row, "col": to}, device_id_type=MESH,
        )

    for i in (0, 1, 3, 6):
        loads[i].wait()
    for m in range(NQ):
        sp[m * BP : m * BP + NB, :] = st_v[m]
        sp[m * BP + NB : (m + 1) * BP, :] = jnp.zeros((BP - NB, E), F32)
    high = mat_v[0:3, :].astype(BF16).astype(F32)
    sp[NQ * BP : NQ * BP + 3, :] = high
    sp[NQ * BP + 3 : NQ * BP + 6, :] = mat_v[0:3, :] - high
    sp[NQ * BP + 6 : KP, :] = jnp.zeros((2, E), F32)
    dof = sp[...].astype(BF16)

    eval_rows = face_rows(fe_v, raw.at[0])

    col_kp = iota((1, KP), 1)
    m_col = steps(col_kp, BP, NQ)
    spread9 = ones_where((iota((BP, 1), 0) == col_kp - BP * m_col) & (col_kp < NQ * BP))
    wide_eval = mm(eval_rows, spread9).astype(BF16)
    row_t = iota((256, 1), 0)
    m_row = steps(row_t, FQ, NQ)
    q_row = row_t - FQ * m_row
    same = (m_row == m_col) & (row_t < NQ * FQ) & (col_kp < NQ * BP)
    carry = (row_t - NQ * FQ == col_kp - NQ * BP) & (col_kp >= NQ * BP)
    for f in range(FACES):
        pick = ones_where(iota((1, 8 * FQ), 1) == 8 * q_row + f)
        weights = jnp.where(same, mm(pick, wide_eval), jnp.where(carry, 1.0, 0.0)).astype(BF16)
        tr[:, f * E : (f + 1) * E] = mm(weights, dof).astype(BF16)

    listed = jnp.transpose(jnp.concatenate([sf_v[0], sf_v[0]], axis=1))
    for p in range(COLS):
        ohs[p * SLOTS : (p + 1) * SLOTS, :] = ones_where(
            listed[0:SLOTS, p : p + 1] == iota((1, FACES * E), 1)
        )
    outgoing = mm_t(ohs[...], tr[...]).astype(BF16)
    for p in range(COLS):
        sendb[p] = outgoing[p * SLOTS : (p + 1) * SLOTS, :]
    xr[col] = jnp.zeros((SLOTS, 256), BF16)

    def wait_column():
        @pl.when(core == 0)
        def _():
            pl.semaphore_wait(barrier, 2 * (COLS - 1) + 1)
            signal(ready_sem, row + 1, col)

        @pl.when(core == 1)
        def _():
            pl.semaphore_wait(ready_sem, 1)

    def wait_plane():
        @pl.when(core == 1)
        def _():
            pl.semaphore_wait(barrier, ROWS - 1)
            signal(ready_sem, row - 1, col)

        @pl.when(core == 0)
        def _():
            pl.semaphore_wait(ready_sem, 1)

    def send_traces():
        @pl.loop(0, COLS - 1)
        def _(i):
            trace_copy(i + jnp.where(i >= col, 1, 0), col).start()

    def send_metric(first, last):
        far = (chip != 0) & (col == 0)

        if first == 0:
            stage.wait()

            @pl.when(far)
            def _():
                metric_copy(1, row).start()

        for dx, dy in FAR[first:last]:
            peer = neighbour(dx, dy)

            @pl.when(jnp.logical_not(far & (peer == 0)))
            def _(peer=peer):
                metric_copy(2 * peer + 1, row).start()

            metric_copy(2 * peer, row).start()
        if last == CHIPS - 1:
            metric_copy(2 * chip + (1 - core), row).start()

    @pl.when(col >= EARLY)
    def _():
        wait_column()
        send_traces()
        wait_plane()
        send_metric(0, CHIPS - 1)

    @pl.when(col < EARLY)
    def _():
        wait_plane()
        send_metric(0, 8)
        wait_column()
        send_traces()
        send_metric(8, CHIPS - 1)

    for i in (2, 4, 5, 7, 8, 9):
        loads[i].wait()

    for m in range(NQ):
        both = jnp.concatenate(
            [sp[m * BP : (m + 1) * BP, :LANES], sp[m * BP : (m + 1) * BP, LANES:]], axis=0
        )
        sb[:, m * LANES : (m + 1) * LANES] = both.astype(BF16)
    tile_col = jnp.where(iota((1, 2 * BP), 1) >= BP, 1, 0)
    twice = ones_where(iota((BP, 1), 0) == iota((1, 2 * BP), 1) - BP * tile_col)
    face_row = iota((8 * FQ, 1), 0)
    eval_mask = ((face_row >> 2) & 1) == tile_col
    face_weights = jnp.where(eval_mask, mm(eval_rows, twice), 0.0).astype(BF16)
    own[...] = mm(face_weights, sb[...]).reshape(FQ, 8, WIDE)
    point_row = iota((256, 1), 0)
    spread_v = ones_where(iota((1, 128), 1) == 4 * (point_row >> 3) + (point_row & 3))
    pad = jnp.zeros((BP - NB, 128), F32)
    eval2 = jnp.concatenate([ve_v[...], pad, ve_v[...], pad], axis=0).astype(BF16)
    vol_mask = ((point_row >> 2) & 1) == tile_col
    vol_weights = jnp.where(vol_mask, mm_t(spread_v, eval2), 0.0).astype(BF16)
    pts[...] = mm(vol_weights, sb[...])
    tile_row = jnp.where(iota((2 * BP, 1), 0) >= BP, 1, 0)
    grads = []
    for d in range(3):
        grad = vg_v[d].astype(F32)
        grads.append(jnp.concatenate([grad, pad, grad, pad], axis=0).astype(BF16))
    for part, weights in ((FIRST, vg_a), (LAST, vg_b)):
        size = 16 * len(part)
        at_row = iota((size, 1), 0)
        source = jnp.zeros((size, 1), I32)
        for i, (dx, dy) in enumerate(part):
            source = jnp.where((at_row >> 4) == i, neighbour(-dx, -dy), source)
        point = 8 * source + 4 * ((at_row >> 3) & 1) + (at_row & 3)
        spread = ones_where(iota((1, 128), 1) == point)
        grad_mask = tile_row == ((iota((1, size), 1) >> 2) & 1)
        for d in range(3):
            weights[:, d * size : (d + 1) * size] = jnp.where(
                grad_mask, mm_t(grads[d], spread), 0.0
            ).astype(BF16)
    twice_t = ones_where(iota((2 * BP, 1), 0) - BP * tile_row == iota((1, BP), 1))
    lift_mask = tile_row == ((iota((1, 8 * FQ), 1) >> 2) & 1)
    lift_rows = face_rows(fl_v, raw.at[1])
    lift = jnp.where(lift_mask, mm_t(twice_t, lift_rows), 0.0).astype(BF16)

    kind, peer, target, turn = nb_v[0], nb_v[1], nb_v[2], nb_v[3]
    face_id = iota((FACES, E), 0) * E + iota((FACES, E), 1)
    code = jnp.where(
        kind == 0, target, jnp.where(kind == 1, FACES * E + peer * SLOTS + target, face_id)
    )
    for f in range(FACES):
        got = mm(tr[...], ones_where(iota((FACES * E, 1), 0) == code[f : f + 1, :]))
        for t in range(2):
            gath[(4 * t + f) * PITCH : (4 * t + f) * PITCH + 256, :] = got[:, t * LANES : (t + 1) * LANES]

        ohr[:, f * E : (f + 1) * E] = ones_where(
            iota((COLS * SLOTS, 1), 0) + FACES * E == code[f : f + 1, :]
        )
    ident = ones_where(iota((256, 1), 0) == iota((1, 256), 1))
    def gathered(r):
        return gath[pl.ds(r, 8, stride=PITCH), :]

    def per_face(i):
        return jnp.concatenate(
            [jnp.broadcast_to(mat_v[i : i + 1, t * LANES : (t + 1) * LANES], (4, LANES)) for t in range(2)],
            axis=0,
        )

    kind8, turn8 = halves(kind), halves(turn)
    l1, g1, w1 = per_face(0), per_face(1), per_face(2)
    speed = jnp.sqrt((l1 + 2.0 * g1) * w1)
    l1, g1, w1 = 0.5 * l1, 0.5 * g1, 0.5 * w1

    @pl.loop(0, FQ)
    def _(q):
        n = [halves(nrm_v[j, q].astype(F32)) for j in range(3)]
        for j in range(3):
            geo8[q, :, j * LANES : (j + 1) * LANES] = n[j]
        geo8[q, :, 3 * LANES : 4 * LANES] = halves(ar_v[q])
        flux = face_flux([own[q, :, m * LANES : (m + 1) * LANES] for m in range(NQ)], l1, g1, w1, n)
        for m in range(NQ):
            base[q, :, m * LANES : (m + 1) * LANES] = -flux[m]

    def all_metric():
        part = recv.at[pl.ds(0, ROWS - 1)]
        return pltpu.make_async_remote_copy(
            src_ref=part, dst_ref=part, send_sem=gsend_sem, recv_sem=grecv_sem.at[0],
            device_id={"row": lax.rem(row + 1, ROWS), "col": col}, device_id_type=MESH,
        )

    def chip_products(dx, dy, i, size, fx):
        src = neighbour(-dx, -dy)
        for a in range(2):
            metric_copy(2 * src + a, 2 * src + a).wait_recv()
        at = pl.multiple_of(16 * src, 16)
        u = [pts[pl.ds(at, 16), m * LANES : (m + 1) * LANES] for m in range(NQ)]
        for d in range(3):
            n = [
                jnp.concatenate(
                    [got8(recv, 2 * src, 3 * d + j), got8(recv, 2 * src + 1, 3 * d + j)], axis=0
                )
                for j in range(3)
            ]
            product = [
                n[0] * u[6],
                n[1] * u[7],
                n[2] * u[8],
                n[0] * u[7] + n[1] * u[6],
                n[1] * u[8] + n[2] * u[7],
                n[0] * u[8] + n[2] * u[6],
                u[0] * n[0] + u[3] * n[1] + u[5] * n[2],
                u[3] * n[0] + u[1] * n[1] + u[4] * n[2],
                u[5] * n[0] + u[4] * n[1] + u[2] * n[2],
            ]
            for m in range(NQ):
                fx[d * size + 16 * i : d * size + 16 * i + 16, m * LANES : (m + 1) * LANES] = product[
                    m
                ].astype(BF16)

    for i, (dx, dy) in enumerate(FIRST):
        chip_products(dx, dy, i, 16 * len(FIRST), fx_a)
    acc[...] = mm(vg_a[...], fx_a[...])

    def products_of_last(first, last):
        for i in range(first, last):
            chip_products(*LAST[i], i, 16 * len(LAST), fx_b)

    traces_late = (col == 1) | (col == 2)

    @pl.when(traces_late)
    def _():
        products_of_last(0, 4)

    def all_traces():
        part = xr.at[pl.ds(0, COLS - 1)]
        return pltpu.make_async_remote_copy(
            src_ref=part, dst_ref=part, send_sem=tsend_sem, recv_sem=trecv_sem,
            device_id={"row": row, "col": lax.rem(col + 1, COLS)}, device_id_type=MESH,
        )

    all_traces().wait_recv()

    xt = mm_t(ident, xr[...].reshape(COLS * SLOTS, 256)).astype(BF16)
    for f in range(FACES):
        got = mm(xt, ohr[:, f * E : (f + 1) * E])
        for t in range(2):
            at = (4 * t + f) * PITCH
            gath[at : at + 256, :] = gath[at : at + 256, :] + got[:, t * LANES : (t + 1) * LANES]

    l2, g2, w2 = [gathered(NQ * FQ + i) + gathered(NQ * FQ + 3 + i) for i in range(3)]
    fastest = 0.5 * jnp.maximum(speed, jnp.sqrt((l2 + 2.0 * g2) * w2))
    sign_v = jnp.where(kind8 == 3, 0.0, 1.0)
    sign_s = jnp.where(kind8 == 2, -1.0, sign_v)
    l2, g2, w2 = 0.5 * l2, 0.5 * g2, 0.5 * w2
    turn_one, turn_two = turn8 == 1, turn8 == 2

    @pl.loop(0, FQ // 3)
    def _(i):
        q0 = 3 * i
        outer = [[], [], []]
        for m in range(NQ):
            g = [gathered(m * FQ + q0 + k) for k in range(3)]
            sign = sign_s if m < 6 else sign_v
            for k in range(3):
                outer[k].append(
                    sign
                    * jnp.where(turn_one, g[(k + 1) % 3], jnp.where(turn_two, g[(k + 2) % 3], g[k]))
                )
        for k in range(3):
            q = q0 + k
            n = [geo8[q, :, j * LANES : (j + 1) * LANES] for j in range(3)]
            penalty = fastest * geo8[q, :, 3 * LANES : 4 * LANES]
            flux = face_flux(outer[k], l2, g2, w2, n)
            for m in range(NQ):
                lanes = slice(m * LANES, (m + 1) * LANES)
                flx[q, :, lanes] = penalty * (own[q, :, lanes] - outer[k][m]) + (base[q, :, lanes] - flux[m])

    surface = mm(lift, flx[...].reshape(8 * FQ, WIDE).astype(BF16))

    @pl.when(jnp.logical_not(traces_late))
    def _():
        products_of_last(0, 4)

    products_of_last(4, len(LAST))

    all_metric().wait_send()
    all_traces().wait_send()
    volume = acc[...] + mm(vg_b[...], fx_b[...])
    for t in range(2):
        rows = slice(t * BP, (t + 1) * BP)
        lanes = slice(t * LANES, (t + 1) * LANES)
        v = [volume[rows, m * LANES : (m + 1) * LANES] for m in range(NQ)]
        l, g, w, step = [mat_v[i : i + 1, lanes] for i in range(4)]
        pressure = l * (v[0] + v[1] + v[2])
        for m in range(NQ):
            if m < 3:
                total = -(pressure + 2.0 * g * v[m])
            elif m < 6:
                total = -g * v[m]
            else:
                total = -w * v[m]
            total = total - surface[rows, m * LANES : (m + 1) * LANES]
            out[m, :, lanes] = st_v[m, :, lanes] + (step * total)[0:NB]


def got8(recv, r, k):
    return recv[r, k].astype(F32).reshape(8, LANES)


def per_device(
    state, geometry, material, neighbours, send_faces, vol_eval, vol_grad, face_eval, face_lift,
    normals, areas,
):
    geometry = jnp.transpose(geometry.reshape(9, 4, 2 * ROWS, LANES), (0, 2, 1, 3))
    face_eval = jnp.transpose(face_eval, (2, 0, 1))
    face_lift = jnp.transpose(face_lift, (2, 0, 1))
    args = (
        state, geometry, material, neighbours, send_faces, vol_eval, vol_grad, face_eval, face_lift,
        normals, areas,
    )
    args = tuple(pltpu.with_memory_space_constraint(a, pltpu.HBM) for a in args)
    staged = [a for i, a in enumerate(args) if i != 1]
    dma = pltpu.SemaphoreType.DMA
    return pl.pallas_call(
        kernel,
        out_shape=jax.ShapeDtypeStruct((NQ, NB, E), F32),
        in_specs=[pl.BlockSpec(memory_space=pl.ANY)] * len(args),
        out_specs=pl.BlockSpec(memory_space=pltpu.VMEM),
        scratch_shapes=[pltpu.VMEM(a.shape, a.dtype) for a in (args[1], *staged)]
        + [
            pltpu.VMEM((ROWS, 9, 2, 4, LANES), BF16),
            pltpu.VMEM((COLS, SLOTS, 256), BF16),
            pltpu.VMEM((COLS, SLOTS, 256), BF16),
            pltpu.VMEM((KP, E), F32),
            pltpu.VMEM((2 * BP, WIDE), BF16),
            pltpu.VMEM((2, 8 * FQ, BP), F32),
            pltpu.VMEM((COLS * SLOTS, FACES * E), BF16),
            pltpu.VMEM((COLS * SLOTS, FACES * E), BF16),
            pltpu.VMEM((256, FACES * E), BF16),
            pltpu.VMEM((256, WIDE), F32),
            pltpu.VMEM((FQ, 8, WIDE), F32),
            pltpu.VMEM((9 * PITCH, LANES), F32),
            pltpu.VMEM((FQ, 8, WIDE), F32),
            pltpu.VMEM((48 * len(FIRST), WIDE), BF16),
            pltpu.VMEM((48 * len(LAST), WIDE), BF16),
            pltpu.VMEM((2 * BP, 48 * len(FIRST)), BF16),
            pltpu.VMEM((2 * BP, 48 * len(LAST)), BF16),
            pltpu.VMEM((2 * BP, WIDE), F32),
            pltpu.VMEM((FQ, 8, WIDE), F32),
            pltpu.VMEM((FQ, 8, 4 * LANES), F32),
            dma((len(args),)), pltpu.SemaphoreType.DMA, dma((ROWS,)), pltpu.SemaphoreType.DMA, pltpu.SemaphoreType.DMA,
            pltpu.SemaphoreType.REGULAR,
        ],
        compiler_params=pltpu.CompilerParams(
            collective_id=0, has_side_effects=True, vmem_limit_bytes=40 * 1024 * 1024
        ),
        name="section",
    )(*args)


def solution(mesh):
    blocks = P(None, None, ("col", "row"))
    in_specs = (
        blocks, P(None, "row", "col"), P(None, ("col", "row")), blocks, P(("col", "row"), None, None),
        P(), P(), P(), P(), P(None, None, None, ("col", "row")), blocks,
    )
    return jax.shard_map(
        per_device, mesh=mesh, in_specs=in_specs, out_specs=blocks, check_vma=False
    )
```
